32 devices in a mesh: dp: 4 (over y, z), ep: 8 (over x, core).
Axes of the slice: x: 4, y: 2, z: 2, core: 2. Of those that a mesh axis runs over, the one named last changes fastest.
The devices are a block of a 4x4x8 slice.
Arguments:
- x_tokens: bfloat16 [4096, 1024], P(('dp', 'ep')), parts along dimension 0
- dy_tokens: bfloat16 [4096, 1024], P(('dp', 'ep')), parts along dimension 0
- expert_ids: int32 [4096, 8], P(('dp', 'ep')), parts along dimension 0
- gate_vals: float32 [4096, 8], P(('dp', 'ep')), parts along dimension 0
- slot_ids: int32 [4096, 8], P(('dp', 'ep')), parts along dimension 0
- w_gate: bfloat16 [32, 1024, 512], P('ep')
- w_down: bfloat16 [32, 512, 1024], P('ep')
- w_up: bfloat16 [32, 1024, 512], P('ep')
Outputs:
- output 1: bfloat16 [4096, 1024], P(('dp', 'ep')), parts along dimension 0
- output 2: float32 [128, 1024, 512], P(('dp', 'ep')), parts along dimension 0
- output 3: float32 [128, 512, 1024], P(('dp', 'ep')), parts along dimension 0
- output 4: float32 [128, 1024, 512], P(('dp', 'ep')), parts along dimension 0
There are 4 independent parts. The reference program is written for one: setup_inputs(seed, part) draws one part's arguments, and reference() takes and returns one part's arrays. A program takes and returns all parts, laid end to end along the dimension named above; an argument that names none is the same for every part.
All inputs are finite; a program needn't handle non-finite values.
Results may differ from the reference program's by a relative error of at most 0.0103867.
Values are sent between devices in bfloat16 or wider.
A program may use at most 768 MiB of HBM per device.

```python
import jax
import jax.numpy as jnp
from jax import lax

D = 1024
FF = 512
EXPERTS = 32
TOP = 8
GROUP = 8
TOK = 128
CAP = 48


def source_routing(src_key):
    key_base, key_offset, key_hot = jax.random.split(src_key, 3)
    stride = EXPERTS // TOP
    base_expert = jax.random.randint(key_base, (TOK,), 0, EXPERTS)
    offset = jax.random.randint(key_offset, (TOK, TOP), 0, stride)
    hot_expert = jax.random.randint(key_hot, (), 0, EXPERTS)
    forced = jnp.arange(TOK) < CAP
    base_expert = jnp.where(forced, hot_expert, base_expert)
    offset = jnp.where(forced[:, None] & (jnp.arange(TOP)[None, :] == 0), 0, offset)
    experts = (base_expert[:, None] + jnp.arange(TOP)[None, :] * stride + offset) % EXPERTS
    n_copy = TOK * TOP
    flat_exp = experts.reshape(n_copy)
    copy_ids = jnp.arange(n_copy)
    sort_order = jnp.argsort(flat_exp * n_copy + copy_ids)
    exp_counts = jnp.zeros((EXPERTS,), jnp.int32).at[flat_exp].add(1)
    exp_starts = jnp.cumsum(exp_counts) - exp_counts
    sorted_rank = copy_ids - exp_starts[flat_exp[sort_order]]
    copy_rank = jnp.zeros((n_copy,), jnp.int32).at[sort_order].set(sorted_rank)
    slots = jnp.where(copy_rank < CAP, copy_rank, -1)
    return experts.astype(jnp.int32), slots.reshape(TOK, TOP).astype(jnp.int32)


def setup_inputs(seed: int = 0, part: int = 0) -> dict:
    root_key = jax.random.key(seed)
    sub_keys = jax.random.split(root_key, 7)
    n_tok = GROUP * TOK
    x_tokens = jax.random.normal(jax.random.fold_in(sub_keys[0], part), (n_tok, D), jnp.float32).astype(jnp.bfloat16)
    dy_tokens = jax.random.normal(jax.random.fold_in(sub_keys[1], part), (n_tok, D), jnp.float32).astype(jnp.bfloat16)
    gate_vals = jax.random.uniform(jax.random.fold_in(sub_keys[2], part), (n_tok, TOP), jnp.float32, 0.3, 1.0)
    src_keys = jax.random.split(jax.random.fold_in(sub_keys[3], part), GROUP)
    expert_ids, slot_ids = jax.vmap(source_routing)(src_keys)
    w_gate = (jax.random.normal(sub_keys[4], (EXPERTS, D, FF), jnp.float32) * D ** -0.5).astype(jnp.bfloat16)
    w_down = (jax.random.normal(sub_keys[5], (EXPERTS, FF, D), jnp.float32) * FF ** -0.5).astype(jnp.bfloat16)
    w_up = (jax.random.normal(sub_keys[6], (EXPERTS, D, FF), jnp.float32) * D ** -0.5).astype(jnp.bfloat16)
    return {'x_tokens': x_tokens, 'dy_tokens': dy_tokens, 'expert_ids': expert_ids.reshape(n_tok, TOP), 'gate_vals': gate_vals, 'slot_ids': slot_ids.reshape(n_tok, TOP), 'w_gate': w_gate, 'w_down': w_down, 'w_up': w_up}


def expert_backward(operands):
    x_rows, dz_rows, w_gate, w_down, w_up = operands
    a_pre = jnp.dot(x_rows, w_gate, preferred_element_type=jnp.float32).astype(jnp.bfloat16).astype(jnp.float32)
    b_pre = jnp.dot(x_rows, w_up, preferred_element_type=jnp.float32).astype(jnp.bfloat16).astype(jnp.float32)
    sigma_a = jax.nn.sigmoid(a_pre)
    silu_a = a_pre * sigma_a
    hidden = (silu_a * b_pre).astype(jnp.bfloat16)
    d_hidden = jnp.dot(dz_rows, w_down.T, preferred_element_type=jnp.float32)
    d_gate = (d_hidden * b_pre * sigma_a * (1.0 + a_pre * (1.0 - sigma_a))).astype(jnp.bfloat16)
    d_up = (d_hidden * silu_a).astype(jnp.bfloat16)
    g_down = jnp.dot(hidden.T, dz_rows, preferred_element_type=jnp.float32)
    g_gate = jnp.dot(x_rows.T, d_gate, preferred_element_type=jnp.float32)
    g_up = jnp.dot(x_rows.T, d_up, preferred_element_type=jnp.float32)
    dx_rows = (jnp.dot(d_gate, w_gate.T, preferred_element_type=jnp.float32) + jnp.dot(d_up, w_up.T, preferred_element_type=jnp.float32)).astype(jnp.bfloat16)
    return dx_rows, g_gate, g_down, g_up


def reference(x_tokens, dy_tokens, expert_ids, gate_vals, slot_ids, w_gate, w_down, w_up):
    n_tok = GROUP * TOK
    n_rows = GROUP * CAP
    n_slot = EXPERTS * n_rows
    source = jnp.arange(n_tok) // TOK
    buf_index = jnp.where(slot_ids >= 0, expert_ids * n_rows + source[:, None] * CAP + slot_ids, n_slot)
    slot_copy = jnp.full((n_slot,), n_tok * TOP, jnp.int32).at[buf_index.reshape(n_tok * TOP)].set(jnp.arange(n_tok * TOP, dtype=jnp.int32), mode='drop')
    slot_tok = slot_copy // TOP
    x_buf = jnp.take(x_tokens, slot_tok, axis=0, mode='fill', fill_value=0).reshape(EXPERTS, n_rows, D)
    gate_slot = jnp.take(gate_vals.reshape(n_tok * TOP), slot_copy, mode='fill', fill_value=0)
    dy_slot = jnp.take(dy_tokens, slot_tok, axis=0, mode='fill', fill_value=0)
    dz_buf = (gate_slot[:, None] * dy_slot).astype(jnp.bfloat16).reshape(EXPERTS, n_rows, D)
    dx_buf, dw_gate, dw_down, dw_up = lax.map(expert_backward, (x_buf, dz_buf, w_gate, w_down, w_up))
    returned = jnp.take(dx_buf.reshape(n_slot, D), buf_index, axis=0, mode='fill', fill_value=0)
    dx_tokens = jnp.sum(returned.astype(jnp.float32), axis=1).astype(jnp.bfloat16)
    return (dx_tokens, dw_gate, dw_down, dw_up)
```

```python
import functools

import jax
import jax.numpy as jnp
from jax import lax
from jax.experimental import pallas as pl
from jax.experimental.pallas import tpu as pltpu
from jax.sharding import PartitionSpec as P

BF = jnp.bfloat16
F32 = jnp.float32
COLS = 256


def slot_capacity(tok_dev, top_k, n_exp):
    return ((3 * tok_dev * top_k) // (2 * n_exp) + 7) // 8 * 8


def dot(a, b, ca=1, cb=0):
    return lax.dot_general(a, b, (((ca,), (cb,)), ((), ())), preferred_element_type=F32)


PASSES = (((0, 0), (0, 1), (2, 0), (2, 1)), ((1, 0), (1, 1), (3, 0), (3, 1)))


def route_kernel(
    n_dev, cap, x_hbm, y_hbm, meta_hbm, w1_hbm, w2_hbm, w3_hbm,
    xr_out, zr_out, h_out, da_out, db_out, own_out, right_out, left_out,
    xb, yb, mb, w1, w2, w3, xr, zr, hb, dab, dbb, dxb, oh, part, ddr, hopr, osum,
    send_sem, recv_sem, load_sem, out_sem,
):
    n_chip = n_dev // 2
    me = lax.axis_index("ep")
    chip, core = me // 2, me % 2
    right = {"ep": ((chip + 1) % n_chip) * 2 + core}
    left = {"ep": ((chip + n_chip - 1) % n_chip) * 2 + core}
    mate = {"ep": chip * 2 + 1 - core}
    n_loc, d_model, d_ff = w1.shape
    tok = x_hbm.shape[0]
    half = tok // 2
    rows = 4 * cap
    halves = (pl.ds(0, half), pl.ds(half, half))

    loads = [
        pltpu.make_async_copy(x_hbm, xb.at[0, 0], load_sem.at[0]),
        pltpu.make_async_copy(y_hbm, yb.at[0, 0], load_sem.at[1]),
        pltpu.make_async_copy(meta_hbm, mb.at[0, 0], load_sem.at[2]),
        pltpu.make_async_copy(w1_hbm, w1, load_sem.at[3]),
        pltpu.make_async_copy(w3_hbm, w3, load_sem.at[4]),
        pltpu.make_async_copy(w2_hbm, w2, load_sem.at[5]),
    ]
    for c in loads:
        c.start()

    barrier = pltpu.get_barrier_semaphore()
    for peer in (right, left, mate):
        pl.semaphore_signal(barrier, inc=1, device_id=peer, device_id_type=pl.DeviceIdType.MESH)
    pl.semaphore_wait(barrier, 3)

    made = []

    def send(src, dst, peer):
        n = len(made)
        c = pltpu.make_async_remote_copy(
            src_ref=src, dst_ref=dst, send_sem=send_sem.at[n], recv_sem=recv_sem.at[n],
            device_id=peer, device_id_type=pl.DeviceIdType.MESH)
        c.start()
        made.append(c)
        return c

    for c in loads[:3]:
        c.wait()

    m_r = send(mb.at[0, 0], mb.at[3, 0], right)
    m_l = send(mb.at[0, 0], mb.at[1, 0], left)
    m_m = send(mb.at[0, 0], mb.at[0, 1], mate)
    x_r = [send(xb.at[0, 0, h], xb.at[3, 0, h], right) for h in halves]
    y_l = [send(yb.at[0, 0, h], yb.at[1, 0, h], left) for h in halves]
    x_m = send(xb.at[0, 0], xb.at[0, 1], mate)
    y_m = send(yb.at[0, 0], yb.at[0, 1], mate)

    m_r.wait_recv()
    m_f = send(mb.at[3, 0], mb.at[2, 0], right)
    m_r2 = send(mb.at[3, 0], mb.at[3, 1], mate)
    m_l.wait_recv()
    m_l2 = send(mb.at[1, 0], mb.at[1, 1], mate)
    x_f, y_f = [], []
    for i, h in enumerate(halves):
        x_r[i].wait_recv()
        x_f.append(send(xb.at[3, 0, h], xb.at[2, 0, h], right))
        y_l[i].wait_recv()
        y_f.append(send(yb.at[1, 0, h], yb.at[2, 0, h], left))
    y_r = send(yb.at[0, 0], yb.at[3, 0], right)
    x_l = send(xb.at[0, 0], xb.at[1, 0], left)
    m_f.wait_recv()
    m_f2 = send(mb.at[2, 0], mb.at[2, 1], mate)
    x_f2, y_f2 = [], []
    for i, h in enumerate(halves):
        x_f[i].wait_recv()
        x_f2.append(send(xb.at[2, 0, h], xb.at[2, 1, h], mate))
        y_f[i].wait_recv()
        y_f2.append(send(yb.at[2, 0, h], yb.at[2, 1, h], mate))
    x_m.wait_recv()
    y_m.wait_recv()
    m_m.wait_recv()

    for c in loads[3:]:
        c.wait()

    row_id = lax.broadcasted_iota(jnp.int32, (n_loc * cap, tok), 0) + me * (n_loc * cap)

    def place(p, i):
        d, k = PASSES[p][i]
        q = 4 * p + i
        keys = mb[d, k, 0:8, :].astype(jnp.int32)
        gates = mb[d, k, 8:16, :]
        hot = jnp.zeros((n_loc * cap, tok), F32)
        gate = jnp.zeros((n_loc * cap, tok), F32)
        for j in range(8):
            hit = keys[j:j + 1, :] == row_id
            hot = jnp.where(hit, 1.0, hot)
            gate = jnp.where(hit, gates[j:j + 1, :], gate)
        gate_row = jnp.sum(gate, axis=1, keepdims=True)
        hot = hot.astype(BF)
        oh[q] = hot
        for n in range(d_model // COLS):
            cols = pl.ds(n * COLS, COLS)
            xv = dot(hot, xb[d, k, :, cols]).astype(BF)
            zv = (dot(hot, yb[d, k, :, cols]) * gate_row).astype(BF)
            for e in range(n_loc):
                xr[e, pl.ds(q * cap, cap), cols] = xv[e * cap:(e + 1) * cap]
                zr[e, pl.ds(q * cap, cap), cols] = zv[e * cap:(e + 1) * cap]

    def experts(p):
        at = pl.ds(p * rows, rows)

        def one(e, carry):
            x_e = xr[e, at, :]
            z_e = zr[e, at, :]
            for n in range(d_ff // COLS):
                cols = pl.ds(n * COLS, COLS)
                a = dot(x_e, w1[e, :, cols]).astype(BF).astype(F32)
                b = dot(x_e, w3[e, :, cols]).astype(BF).astype(F32)
                dh = dot(z_e, w2[e, cols, :], 1, 1)
                sg = jax.nn.sigmoid(a)
                act = a * sg
                hb[e, at, cols] = (act * b).astype(BF)
                dab[e, at, cols] = (dh * b * sg * (1.0 + a * (1.0 - sg))).astype(BF)
                dbb[e, at, cols] = (dh * act).astype(BF)
            da = dab[e, at, :]
            db = dbb[e, at, :]
            for n in range(d_model // COLS):
                cols = pl.ds(n * COLS, COLS)
                dxb[e, :, cols] = (dot(da, w1[e, cols, :], 1, 1) + dot(db, w3[e, cols, :], 1, 1)).astype(BF)
            return carry

        lax.fori_loop(0, n_loc, one, 0)

    def combine(p, i):
        q = 4 * p + i
        for n in range(d_model // COLS):
            cols = pl.ds(n * COLS, COLS)
            back = jnp.concatenate([dxb[e, pl.ds(i * cap, cap), cols] for e in range(n_loc)], axis=0)
            part[q, :, cols] = dot(oh[q], back, 0, 0)

    def stash(p):
        at = pl.ds(p * rows, rows)
        out = []
        for t, (src, dst) in enumerate(((xr, xr_out), (zr, zr_out), (hb, h_out), (dab, da_out), (dbb, db_out))):
            c = pltpu.make_async_copy(src.at[:, at, :], dst.at[:, at, :], out_sem.at[5 * p + t])
            c.start()
            out.append(c)
        return out

    place(0, 0)
    place(0, 1)
    m_f2.wait_recv()
    for i in range(2):
        x_f2[i].wait_recv()
        y_f2[i].wait_recv()
    place(0, 2)
    place(0, 3)
    experts(0)
    outs = stash(0)

    y_r.wait_recv()
    y_r2 = send(yb.at[3, 0], yb.at[3, 1], mate)
    x_l.wait_recv()
    x_l2 = send(xb.at[1, 0], xb.at[1, 1], mate)
    x_r2 = send(xb.at[3, 0], xb.at[3, 1], mate)
    y_l2 = send(yb.at[1, 0], yb.at[1, 1], mate)

    combine(0, 3)
    d_opp = send(part.at[3], ddr.at[1], mate)
    combine(0, 2)
    combine(0, 1)
    d_own = send(part.at[1], ddr.at[0], mate)
    combine(0, 0)
    d_opp.wait_recv()
    osum[...] = part[2] + ddr[1]
    hop_r = send(osum.at[pl.ds(0, half)], hopr.at[0], right)
    hop_l = send(osum.at[pl.ds(half, half)], hopr.at[1], left)

    m_r2.wait_recv()
    m_l2.wait_recv()
    place(1, 0)
    place(1, 2)
    y_r2.wait_recv()
    x_l2.wait_recv()
    x_r2.wait_recv()
    y_l2.wait_recv()
    place(1, 1)
    place(1, 3)
    experts(1)
    outs += stash(1)
    combine(1, 1)
    d_right = send(part.at[5], ddr.at[2], mate)
    combine(1, 3)
    d_left = send(part.at[7], ddr.at[3], mate)
    combine(1, 0)
    combine(1, 2)
    d_own.wait_recv()
    part[0] += ddr[0]
    d_right.wait_recv()
    d_left.wait_recv()
    hop_r.wait_recv()
    hop_l.wait_recv()
    part[4] += ddr[2]
    part[6] += ddr[3]
    part[4, pl.ds(0, half)] += hopr[0]
    part[6, pl.ds(half, half)] += hopr[1]
    for t, (q, dst) in enumerate(((0, own_out), (4, right_out), (6, left_out))):
        c = pltpu.make_async_copy(part.at[q], dst, out_sem.at[10 + t])
        c.start()
        outs.append(c)
    for c in outs:
        c.wait()
    for c in made:
        c.wait_send()


def route(n_dev, cap, x, y, meta, w1, w2, w3):
    n_loc, d_model, d_ff = w1.shape
    tok = x.shape[0]
    n_rows = n_dev * cap
    any_spec = pl.BlockSpec(memory_space=pl.ANY)
    flops = 2 * n_loc * n_rows * d_model * d_ff * 5
    return pl.pallas_call(
        functools.partial(route_kernel, n_dev, cap),
        out_shape=(
            jax.ShapeDtypeStruct((n_loc, n_rows, d_model), BF),
            jax.ShapeDtypeStruct((n_loc, n_rows, d_model), BF),
            jax.ShapeDtypeStruct((n_loc, n_rows, d_ff), BF),
            jax.ShapeDtypeStruct((n_loc, n_rows, d_ff), BF),
            jax.ShapeDtypeStruct((n_loc, n_rows, d_ff), BF),
            jax.ShapeDtypeStruct((tok, d_model), F32),
            jax.ShapeDtypeStruct((tok, d_model), F32),
            jax.ShapeDtypeStruct((tok, d_model), F32),
        ),
        in_specs=[any_spec] * 6,
        out_specs=[any_spec] * 8,
        scratch_shapes=[
            pltpu.VMEM((4, 2, tok, d_model), BF),
            pltpu.VMEM((4, 2, tok, d_model), BF),
            pltpu.VMEM((4, 2, 16, tok), F32),
            pltpu.VMEM(w1.shape, BF),
            pltpu.VMEM(w2.shape, BF),
            pltpu.VMEM(w3.shape, BF),
            pltpu.VMEM((n_loc, n_rows, d_model), BF),
            pltpu.VMEM((n_loc, n_rows, d_model), BF),
            pltpu.VMEM((n_loc, n_rows, d_ff), BF),
            pltpu.VMEM((n_loc, n_rows, d_ff), BF),
            pltpu.VMEM((n_loc, n_rows, d_ff), BF),
            pltpu.VMEM((n_loc, 4 * cap, d_model), BF),
            pltpu.VMEM((8, n_loc * cap, tok), BF),
            pltpu.VMEM((8, tok, d_model), F32),
            pltpu.VMEM((4, tok, d_model), F32),
            pltpu.VMEM((2, tok // 2, d_model), F32),
            pltpu.VMEM((tok, d_model), F32),
            pltpu.SemaphoreType.DMA((40,)),
            pltpu.SemaphoreType.DMA((40,)),
            pltpu.SemaphoreType.DMA((6,)),
            pltpu.SemaphoreType.DMA((13,)),
        ],
        compiler_params=pltpu.CompilerParams(
            collective_id=0, has_side_effects=True, vmem_limit_bytes=56 * 1024 * 1024),
        cost_estimate=pl.CostEstimate(flops=flops, bytes_accessed=24 * 1024 * 1024, transcendentals=0),
        name="route",
    )(x, y, meta, w1, w2, w3)


def grad_kernel(x_ref, z_ref, h_ref, da_ref, db_ref, g1_ref, g2_ref, g3_ref):
    x = x_ref[0]
    g1_ref[0] = dot(x, da_ref[0], 0, 0)
    g3_ref[0] = dot(x, db_ref[0], 0, 0)
    g2_ref[0] = dot(h_ref[0], z_ref[0], 0, 0)


def grads(xr, zr, h, da, db, parts=2):
    n_loc, n_rows, d_model = xr.shape
    d_ff = h.shape[2]
    bm, bf = d_model // parts, d_ff // parts
    full = lambda width: pl.BlockSpec((1, n_rows, width), lambda e, i: (e, 0, 0))
    part = lambda width: pl.BlockSpec((1, n_rows, width), lambda e, i: (e, 0, i))
    return pl.pallas_call(
        grad_kernel,
        grid=(n_loc, parts),
        in_specs=[part(bm), full(d_model), part(bf), full(d_ff), full(d_ff)],
        out_specs=[
            pl.BlockSpec((1, bm, d_ff), lambda e, i: (e, i, 0)),
            pl.BlockSpec((1, bf, d_model), lambda e, i: (e, i, 0)),
            pl.BlockSpec((1, bm, d_ff), lambda e, i: (e, i, 0)),
        ],
        out_shape=(
            jax.ShapeDtypeStruct((n_loc, d_model, d_ff), F32),
            jax.ShapeDtypeStruct((n_loc, d_ff, d_model), F32),
            jax.ShapeDtypeStruct((n_loc, d_model, d_ff), F32),
        ),
        compiler_params=pltpu.CompilerParams(
            dimension_semantics=("arbitrary", "arbitrary"), vmem_limit_bytes=60 * 1024 * 1024),
        cost_estimate=pl.CostEstimate(
            flops=6 * n_loc * n_rows * d_model * d_ff, bytes_accessed=36 * 1024 * 1024, transcendentals=0),
        name="grads",
    )(xr, zr, h, da, db)


def solution(mesh):
    n_dev = mesh.shape["ep"]
    n_chip = n_dev // 2
    to_right = [(i, ((i // 2 + 1) % n_chip) * 2 + i % 2) for i in range(n_dev)]
    to_left = [(j, i) for i, j in to_right]

    def local_step(x_loc, dy_loc, ids_loc, gate_loc, slot_loc, w_gate, w_down, w_up):
        tok_dev, top_k = ids_loc.shape
        n_exp = w_gate.shape[0] * n_dev
        cap = slot_capacity(tok_dev, top_k, n_exp)
        key = jnp.where(slot_loc >= 0, ids_loc * cap + slot_loc, -1)
        meta = jnp.concatenate([key.astype(F32).T, gate_loc.T], axis=0)
        xr, zr, h, da, db, own, right, left = route(n_dev, cap, x_loc, dy_loc, meta, w_gate, w_down, w_up)
        from_left = lax.ppermute(right, "ep", to_right)
        from_right = lax.ppermute(left, "ep", to_left)
        g_gate, g_down, g_up = grads(xr, zr, h, da, db)
        dx = (own + from_left + from_right).astype(BF)
        return dx, g_gate, g_down, g_up

    tok_spec = P(("dp", "ep"), None)
    w_spec = P("ep", None, None)
    grad_spec = P(("dp", "ep"), None, None)
    return jax.shard_map(
        local_step, mesh=mesh,
        in_specs=(tok_spec, tok_spec, tok_spec, tok_spec, tok_spec, w_spec, w_spec, w_spec),
        out_specs=(tok_spec, grad_spec, grad_spec, grad_spec), check_vma=False)
```

```python
import functools

import jax
import jax.numpy as jnp
from jax import lax
from jax.experimental import pallas as pl
from jax.experimental.pallas import tpu as pltpu
from jax.sharding import PartitionSpec as P

BF = jnp.bfloat16
F32 = jnp.float32
COLS = 256


def slot_capacity(tok_dev, top_k, n_exp):
    return ((3 * tok_dev * top_k) // (2 * n_exp) + 7) // 8 * 8


def dot(a, b, ca=1, cb=0):
    return lax.dot_general(a, b, (((ca,), (cb,)), ((), ())), preferred_element_type=F32)


PASSES = (((0, 0), (0, 1)), ((2, 0), (2, 1)), ((1, 0), (1, 1), (3, 0), (3, 1)))
FIRST = (0, 2, 4)


def route_kernel(
    n_dev, cap, x_hbm, y_hbm, ids_hbm, slots_hbm, gates_hbm, w1_hbm, w2_hbm, w3_hbm,
    xr, zr, hb, dab, dbb, own_out, right_out, left_out,
    xb, yb, mb, w1, w2, w3, dxb, oh, part, ddr, hopr, osum, ids, slots, gates,
    send_sem, recv_sem, load_sem,
):
    n_chip = n_dev // 2
    me = lax.axis_index("ep")
    chip, core = me // 2, me % 2
    right = {"ep": ((chip + 1) % n_chip) * 2 + core}
    left = {"ep": ((chip + n_chip - 1) % n_chip) * 2 + core}
    mate = {"ep": chip * 2 + 1 - core}
    n_loc, d_model, d_ff = w1.shape
    top_k, tok = ids.shape
    half = tok // 2
    halves = (pl.ds(0, half), pl.ds(half, half))

    loads = [
        pltpu.make_async_copy(src, dst, load_sem.at[i])
        for i, (src, dst) in enumerate((
            (x_hbm, xb.at[0, 0]), (y_hbm, yb.at[0, 0]), (ids_hbm, ids), (slots_hbm, slots), (gates_hbm, gates),
            (w1_hbm, w1), (w3_hbm, w3), (w2_hbm, w2)))
    ]
    for c in loads[:5]:
        c.start()

    barrier = pltpu.get_barrier_semaphore()
    for peer in (right, left, mate):
        pl.semaphore_signal(barrier, inc=1, device_id=peer, device_id_type=pl.DeviceIdType.MESH)

    for c in loads[2:5]:
        c.wait()
    mb[0, 0, 0:top_k, :] = jnp.where(slots[...] >= 0, ids[...] * cap + slots[...], -1).astype(F32)
    mb[0, 0, top_k:2 * top_k, :] = gates[...]

    for c in loads[:2]:
        c.wait()
    pl.semaphore_wait(barrier, 3)

    made = []

    def send(src, dst, peer):
        n = len(made)
        c = pltpu.make_async_remote_copy(
            src_ref=src, dst_ref=dst, send_sem=send_sem.at[n], recv_sem=recv_sem.at[n],
            device_id=peer, device_id_type=pl.DeviceIdType.MESH)
        c.start()
        made.append(c)
        return c

    x_r, y_l = [], []
    for h in halves:
        x_r.append(send(xb.at[0, 0, h], xb.at[3, 0, h], right))
        y_l.append(send(yb.at[0, 0, h], yb.at[1, 0, h], left))
    x_m = send(xb.at[0, 0], xb.at[0, 1], mate)
    m_m = send(mb.at[0, 0], mb.at[0, 1], mate)
    y_m = send(yb.at[0, 0], yb.at[0, 1], mate)
    m_r = send(mb.at[0, 0], mb.at[3, 0], right)
    m_l = send(mb.at[0, 0], mb.at[1, 0], left)
    for c in loads[5:]:
        c.start()

    row_id = lax.broadcasted_iota(jnp.int32, (n_loc * cap, tok), 0) + me * (n_loc * cap)

    def place(p, i):
        d, k = PASSES[p][i]
        q = FIRST[p] + i
        keys = mb[d, k, 0:top_k, :].astype(jnp.int32)
        gate_of = mb[d, k, top_k:2 * top_k, :]
        hot = jnp.zeros((n_loc * cap, tok), F32)
        gate = jnp.zeros((n_loc * cap, tok), F32)
        for j in range(top_k):
            hit = keys[j:j + 1, :] == row_id
            hot = jnp.where(hit, 1.0, hot)
            gate = jnp.where(hit, gate_of[j:j + 1, :], gate)
        gate_row = jnp.sum(gate, axis=1, keepdims=True)
        hot = hot.astype(BF)
        oh[q] = hot
        for n in range(d_model // COLS):
            cols = pl.ds(n * COLS, COLS)
            xv = dot(hot, xb[d, k, :, cols]).astype(BF)
            zv = (dot(hot, yb[d, k, :, cols]) * gate_row).astype(BF)
            for e in range(n_loc):
                xr[e, pl.ds(q * cap, cap), cols] = xv[e * cap:(e + 1) * cap]
                zr[e, pl.ds(q * cap, cap), cols] = zv[e * cap:(e + 1) * cap]

    def experts(p, lo, hi):
        rows = len(PASSES[p]) * cap
        at = pl.ds(FIRST[p] * cap, rows)

        def one(e, carry):
            x_e = xr[e, at, :]
            z_e = zr[e, at, :]
            for n in range(d_ff // COLS):
                cols = pl.ds(n * COLS, COLS)
                a = dot(x_e, w1[e, :, cols]).astype(BF).astype(F32)
                b = dot(x_e, w3[e, :, cols]).astype(BF).astype(F32)
                dh = dot(z_e, w2[e, cols, :], 1, 1)
                sg = jax.nn.sigmoid(a)
                act = a * sg
                hb[e, at, cols] = (act * b).astype(BF)
                dab[e, at, cols] = (dh * b * sg * (1.0 + a * (1.0 - sg))).astype(BF)
                dbb[e, at, cols] = (dh * act).astype(BF)
            da = dab[e, at, :]
            db = dbb[e, at, :]
            for n in range(d_model // COLS):
                cols = pl.ds(n * COLS, COLS)
                dxb[e, pl.ds(0, rows), cols] = (
                    dot(da, w1[e, cols, :], 1, 1) + dot(db, w3[e, cols, :], 1, 1)).astype(BF)
            return carry

        lax.fori_loop(lo, hi, one, 0)

    def combine(p, i):
        q = FIRST[p] + i
        for n in range(d_model // COLS):
            cols = pl.ds(n * COLS, COLS)
            back = jnp.concatenate([dxb[e, pl.ds(i * cap, cap), cols] for e in range(n_loc)], axis=0)
            part[q, :, cols] = dot(oh[q], back, 0, 0)

    def forward(i):
        x_r[i].wait_recv()
        x_f.append(send(xb.at[3, 0, halves[i]], xb.at[2, 0, halves[i]], right))
        y_l[i].wait_recv()
        y_f.append(send(yb.at[1, 0, halves[i]], yb.at[2, 0, halves[i]], left))

    x_f, y_f = [], []
    mid = n_loc // 2
    place(0, 0)
    for c in loads[5:]:
        c.wait()
    m_m.wait_recv()
    x_m.wait_recv()
    y_m.wait_recv()
    place(0, 1)
    experts(0, 0, mid)
    forward(0)
    experts(0, mid, n_loc)
    forward(1)
    m_r.wait_recv()
    m_f = send(mb.at[3, 0], mb.at[2, 0], right)
    y_r = send(yb.at[0, 0], yb.at[3, 0], right)
    x_l = send(xb.at[0, 0], xb.at[1, 0], left)
    m_l.wait_recv()
    early = [
        send(mb.at[3, 0], mb.at[3, 1], mate),
        send(mb.at[1, 0], mb.at[1, 1], mate),
        send(xb.at[3, 0], xb.at[3, 1], mate),
        send(yb.at[1, 0], yb.at[1, 1], mate),
    ]
    combine(0, 1)
    d_own = send(part.at[1], ddr.at[0], mate)
    combine(0, 0)

    opp = []
    for i, h in enumerate(halves):
        x_f[i].wait_recv()
        opp.append(send(xb.at[2, 0, h], xb.at[2, 1, h], mate))
        y_f[i].wait_recv()
        opp.append(send(yb.at[2, 0, h], yb.at[2, 1, h], mate))
    m_f.wait_recv()
    opp.append(send(mb.at[2, 0], mb.at[2, 1], mate))
    place(1, 0)
    for c in opp:
        c.wait_recv()
    place(1, 1)
    experts(1, 0, n_loc - 1)
    y_r.wait_recv()
    y_r2 = send(yb.at[3, 0], yb.at[3, 1], mate)
    x_l.wait_recv()
    x_l2 = send(xb.at[1, 0], xb.at[1, 1], mate)
    experts(1, n_loc - 1, n_loc)
    combine(1, 1)
    d_opp = send(part.at[3], ddr.at[1], mate)
    combine(1, 0)
    place(2, 0)
    place(2, 2)
    d_opp.wait_recv()
    osum[...] = part[2] + ddr[1]
    hop_r = send(osum.at[pl.ds(0, half)], hopr.at[0], right)
    hop_l = send(osum.at[pl.ds(half, half)], hopr.at[1], left)
    for c in early:
        c.wait_recv()
    y_r2.wait_recv()
    x_l2.wait_recv()
    place(2, 1)
    place(2, 3)
    experts(2, 0, n_loc)
    combine(2, 1)
    d_right = send(part.at[5], ddr.at[2], mate)
    combine(2, 3)
    d_left = send(part.at[7], ddr.at[3], mate)
    combine(2, 0)
    combine(2, 2)
    d_own.wait_recv()
    own_out[...] = part[0] + ddr[0]
    hop_r.wait_recv()
    hop_l.wait_recv()
    part[4, pl.ds(0, half)] += hopr[0]
    part[6, pl.ds(half, half)] += hopr[1]
    d_right.wait_recv()
    right_out[...] = part[4] + ddr[2]
    d_left.wait_recv()
    left_out[...] = part[6] + ddr[3]
    for c in made:
        c.wait_send()


def route(n_dev, cap, x, y, ids, slots, gates, w1, w2, w3):
    n_loc, d_model, d_ff = w1.shape
    top_k, tok = ids.shape
    n_rows = n_dev * cap
    hbm = pl.BlockSpec(memory_space=pltpu.HBM)
    vmem = pl.BlockSpec(memory_space=pltpu.VMEM)
    flops = 2 * n_loc * n_rows * d_model * d_ff * 5
    return pl.pallas_call(
        functools.partial(route_kernel, n_dev, cap),
        out_shape=(
            jax.ShapeDtypeStruct((n_loc, n_rows, d_model), BF),
            jax.ShapeDtypeStruct((n_loc, n_rows, d_model), BF),
            jax.ShapeDtypeStruct((n_loc, n_rows, d_ff), BF),
            jax.ShapeDtypeStruct((n_loc, n_rows, d_ff), BF),
            jax.ShapeDtypeStruct((n_loc, n_rows, d_ff), BF),
            jax.ShapeDtypeStruct((tok, d_model), F32),
            jax.ShapeDtypeStruct((tok, d_model), F32),
            jax.ShapeDtypeStruct((tok, d_model), F32),
        ),
        in_specs=[hbm] * 8,
        out_specs=[vmem] * 8,
        scratch_shapes=[
            pltpu.VMEM((4, 2, tok, d_model), BF),
            pltpu.VMEM((4, 2, tok, d_model), BF),
            pltpu.VMEM((4, 2, 2 * top_k, tok), F32),
            pltpu.VMEM(w1.shape, BF),
            pltpu.VMEM(w2.shape, BF),
            pltpu.VMEM(w3.shape, BF),
            pltpu.VMEM((n_loc, 4 * cap, d_model), BF),
            pltpu.VMEM((8, n_loc * cap, tok), BF),
            pltpu.VMEM((8, tok, d_model), F32),
            pltpu.VMEM((4, tok, d_model), F32),
            pltpu.VMEM((2, tok // 2, d_model), F32),
            pltpu.VMEM((tok, d_model), F32),
            pltpu.VMEM((top_k, tok), jnp.int32),
            pltpu.VMEM((top_k, tok), jnp.int32),
            pltpu.VMEM((top_k, tok), F32),
            pltpu.SemaphoreType.DMA((40,)),
            pltpu.SemaphoreType.DMA((40,)),
            pltpu.SemaphoreType.DMA((8,)),
        ],
        compiler_params=pltpu.CompilerParams(
            collective_id=0, has_side_effects=True, vmem_limit_bytes=36 * 1024 * 1024),
        cost_estimate=pl.CostEstimate(flops=flops, bytes_accessed=14 * 1024 * 1024, transcendentals=0),
        name="route",
    )(*(pltpu.with_memory_space_constraint(v, pltpu.HBM) for v in (x, y, ids, slots, gates, w1, w2, w3)))


def grad_kernel(x_ref, z_ref, h_ref, da_ref, db_ref, g1_ref, g2_ref, g3_ref):
    x = x_ref[0]
    g1_ref[0] = dot(x, da_ref[0], 0, 0)
    g3_ref[0] = dot(x, db_ref[0], 0, 0)
    g2_ref[0] = dot(h_ref[0], z_ref[0], 0, 0)


def grads(xr, zr, h, da, db, parts=2):
    n_loc, n_rows, d_model = xr.shape
    d_ff = h.shape[2]
    bm, bf = d_model // parts, d_ff // parts
    full = lambda width: pl.BlockSpec((1, n_rows, width), lambda e, i: (e, 0, 0))
    part = lambda width: pl.BlockSpec((1, n_rows, width), lambda e, i: (e, 0, i))
    return pl.pallas_call(
        grad_kernel,
        grid=(n_loc, parts),
        in_specs=[part(bm), full(d_model), part(bf), full(d_ff), full(d_ff)],
        out_specs=[
            pl.BlockSpec((1, bm, d_ff), lambda e, i: (e, i, 0)),
            pl.BlockSpec((1, bf, d_model), lambda e, i: (e, i, 0)),
            pl.BlockSpec((1, bm, d_ff), lambda e, i: (e, i, 0)),
        ],
        out_shape=(
            jax.ShapeDtypeStruct((n_loc, d_model, d_ff), F32),
            jax.ShapeDtypeStruct((n_loc, d_ff, d_model), F32),
            jax.ShapeDtypeStruct((n_loc, d_model, d_ff), F32),
        ),
        compiler_params=pltpu.CompilerParams(
            dimension_semantics=("arbitrary", "arbitrary"), vmem_limit_bytes=20 * 1024 * 1024),
        cost_estimate=pl.CostEstimate(
            flops=6 * n_loc * n_rows * d_model * d_ff, bytes_accessed=26 * 1024 * 1024, transcendentals=0),
        name="grads",
    )(xr, zr, h, da, db)


def solution(mesh):
    n_dev = mesh.shape["ep"]
    n_chip = n_dev // 2
    to_right = [(i, ((i // 2 + 1) % n_chip) * 2 + i % 2) for i in range(n_dev)]
    to_left = [(j, i) for i, j in to_right]

    def local_step(x_loc, dy_loc, ids_loc, gate_loc, slot_loc, w_gate, w_down, w_up):
        tok_dev, top_k = ids_loc.shape
        n_exp = w_gate.shape[0] * n_dev
        cap = slot_capacity(tok_dev, top_k, n_exp)
        xr, zr, h, da, db, own, right, left = route(
            n_dev, cap, x_loc, dy_loc, ids_loc.T, slot_loc.T, gate_loc.T, w_gate, w_down, w_up)
        from_left = lax.ppermute(right, "ep", to_right)
        from_right = lax.ppermute(left, "ep", to_left)
        g_gate, g_down, g_up = grads(xr, zr, h, da, db)
        dx = (own + from_left + from_right).astype(BF)
        return dx, g_gate, g_down, g_up

    tok_spec = P(("dp", "ep"), None)
    w_spec = P("ep", None, None)
    grad_spec = P(("dp", "ep"), None, None)
    return jax.shard_map(
        local_step, mesh=mesh,
        in_specs=(tok_spec, tok_spec, tok_spec, tok_spec, tok_spec, w_spec, w_spec, w_spec),
        out_specs=(tok_spec, grad_spec, grad_spec, grad_spec), check_vma=False)
```

```python
import functools

import jax
import jax.numpy as jnp
from jax import lax
from jax.experimental import pallas as pl
from jax.experimental.pallas import tpu as pltpu
from jax.sharding import PartitionSpec as P

BF = jnp.bfloat16
F32 = jnp.float32
COLS = 256


def slot_capacity(tok_dev, top_k, n_exp):
    return ((3 * tok_dev * top_k) // (2 * n_exp) + 7) // 8 * 8


def dot(a, b, ca=1, cb=0):
    return lax.dot_general(a, b, (((ca,), (cb,)), ((), ())), preferred_element_type=F32)


PASSES = (((0, 0), (0, 1)), ((2, 0), (2, 1)), ((1, 0), (1, 1), (3, 0), (3, 1)))
FIRST = (0, 2, 4)
LAG = 2


def route_kernel(
    n_dev, cap, x_hbm, y_hbm, ids_hbm, slots_hbm, gates_hbm, w1_hbm, w2_hbm, w3_hbm,
    xr, zr, hb, dab, dbb, own_out, right_out, left_out,
    xb, yb, mb, w1, w2, w3, dxb, oht, part, ddr, hopr, osum, ids, slots, gates,
    send_sem, recv_sem, load_sem,
):
    n_chip = n_dev // 2
    me = lax.axis_index("ep")
    chip, core = me // 2, me % 2
    right = {"ep": ((chip + 1) % n_chip) * 2 + core}
    left = {"ep": ((chip + n_chip - 1) % n_chip) * 2 + core}
    mate = {"ep": chip * 2 + 1 - core}
    n_loc, d_model, d_ff = w1.shape
    top_k, tok = ids.shape
    half = tok // 2
    halves = (pl.ds(0, half), pl.ds(half, half))

    loads = [
        pltpu.make_async_copy(src, dst, load_sem.at[i])
        for i, (src, dst) in enumerate((
            (x_hbm, xb.at[0, 0]), (y_hbm, yb.at[0, 0]), (ids_hbm, ids), (slots_hbm, slots), (gates_hbm, gates),
            (w1_hbm, w1), (w3_hbm, w3), (w2_hbm, w2)))
    ]
    for c in loads[:5]:
        c.start()

    barrier = pltpu.get_barrier_semaphore()
    for peer in (right, left, mate):
        pl.semaphore_signal(barrier, inc=1, device_id=peer, device_id_type=pl.DeviceIdType.MESH)

    for c in loads[2:5]:
        c.wait()
    mb[0, 0, 0:top_k, :] = jnp.where(slots[...] >= 0, ids[...] * cap + slots[...], -1).astype(F32)
    mb[0, 0, top_k:2 * top_k, :] = gates[...]

    for c in loads[:2]:
        c.wait()
    for c in loads[5:]:
        c.start()
    pl.semaphore_wait(barrier, 3)

    made = []

    def send(src, dst, peer):
        n = len(made)
        c = pltpu.make_async_remote_copy(
            src_ref=src, dst_ref=dst, send_sem=send_sem.at[n], recv_sem=recv_sem.at[n],
            device_id=peer, device_id_type=pl.DeviceIdType.MESH)
        c.start()
        made.append(c)
        return c

    x_r, y_l = [], []
    for h in halves:
        x_r.append(send(xb.at[0, 0, h], xb.at[3, 0, h], right))
        y_l.append(send(yb.at[0, 0, h], yb.at[1, 0, h], left))
    x_m = send(xb.at[0, 0], xb.at[0, 1], mate)
    m_m = send(mb.at[0, 0], mb.at[0, 1], mate)
    y_m = send(yb.at[0, 0], yb.at[0, 1], mate)
    m_r = send(mb.at[0, 0], mb.at[3, 0], right)
    m_l = send(mb.at[0, 0], mb.at[1, 0], left)

    row_id = lax.broadcasted_iota(jnp.int32, (n_loc * cap, tok), 0) + me * (n_loc * cap)

    def place(p, i):
        d, k = PASSES[p][i]
        q = FIRST[p] + i
        keys = mb[d, k, 0:top_k, :].astype(jnp.int32)
        gate_of = mb[d, k, top_k:2 * top_k, :]
        hot = jnp.zeros((n_loc * cap, tok), F32)
        gate = jnp.zeros((n_loc * cap, tok), F32)
        for j in range(top_k):
            hit = keys[j:j + 1, :] == row_id
            hot = jnp.where(hit, 1.0, hot)
            gate = jnp.where(hit, gate_of[j:j + 1, :], gate)
        gate_row = jnp.sum(gate, axis=1, keepdims=True)
        hot = hot.astype(BF)
        oht[q] = hot.T
        for n in range(d_model // COLS):
            cols = pl.ds(n * COLS, COLS)
            xv = dot(hot, xb[d, k, :, cols]).astype(BF)
            zv = (dot(hot, yb[d, k, :, cols]) * gate_row).astype(BF)
            for e in range(n_loc):
                xr[e, pl.ds(q * cap, cap), cols] = xv[e * cap:(e + 1) * cap]
                zr[e, pl.ds(q * cap, cap), cols] = zv[e * cap:(e + 1) * cap]

    def inner(p, e):
        at = pl.ds(FIRST[p] * cap, len(PASSES[p]) * cap)
        x_e = xr[e, at, :]
        z_e = zr[e, at, :]
        for n in range(d_ff // COLS):
            cols = pl.ds(n * COLS, COLS)
            a = dot(x_e, w1[e, :, cols]).astype(BF).astype(F32)
            b = dot(x_e, w3[e, :, cols]).astype(BF).astype(F32)
            dh = dot(z_e, w2[e, cols, :], 1, 1)
            sg = jax.nn.sigmoid(a)
            act = a * sg
            hb[e, at, cols] = (act * b).astype(BF)
            dab[e, at, cols] = (dh * b * sg * (1.0 + a * (1.0 - sg))).astype(BF)
            dbb[e, at, cols] = (dh * act).astype(BF)

    def experts(p, lo, hi):
        lax.fori_loop(lo, hi, lambda e, c: (inner(p, e), c)[1], 0)

    def back(p, cols):
        rows = len(PASSES[p]) * cap
        at = pl.ds(FIRST[p] * cap, rows)

        def one(e, carry):
            dxb[e, pl.ds(0, rows), cols] = (
                dot(dab[e, at, :], w1[e, cols, :], 1, 1) + dot(dbb[e, at, :], w3[e, cols, :], 1, 1)).astype(BF)
            return carry

        for e in range(n_loc):
            one(e, 0)

    def combine(p, i, cols):
        q = FIRST[p] + i
        rows = jnp.concatenate([dxb[e, pl.ds(i * cap, cap), cols] for e in range(n_loc)], axis=0)
        part[q, :, cols] = dot(oht[q], rows)

    def forward(i):
        x_r[i].wait_recv()
        x_f.append(send(xb.at[3, 0, halves[i]], xb.at[2, 0, halves[i]], right))
        y_l[i].wait_recv()
        y_f.append(send(yb.at[1, 0, halves[i]], yb.at[2, 0, halves[i]], left))

    n_cols = d_model // COLS
    chunks = [pl.ds(n * COLS, COLS) for n in range(n_cols)]
    x_f, y_f = [], []
    mid = n_loc // 2
    place(0, 0)
    m_m.wait_recv()
    x_m.wait_recv()
    y_m.wait_recv()
    place(0, 1)
    forward(0)
    for c in loads[5:]:
        c.wait()
    experts(0, 0, mid)
    forward(1)
    m_r.wait_recv()
    m_f = send(mb.at[3, 0], mb.at[2, 0], right)
    y_r = send(yb.at[0, 0], yb.at[3, 0], right)
    x_l = send(xb.at[0, 0], xb.at[1, 0], left)
    m_l.wait_recv()
    early = [
        send(mb.at[3, 0], mb.at[3, 1], mate),
        send(mb.at[1, 0], mb.at[1, 1], mate),
        send(xb.at[3, 0], xb.at[3, 1], mate),
        send(yb.at[1, 0], yb.at[1, 1], mate),
    ]
    experts(0, mid, n_loc)
    for cols in chunks:
        back(0, cols)
        combine(0, 1, cols)
    d_own = send(part.at[1], ddr.at[0], mate)
    for cols in chunks:
        combine(0, 0, cols)
    d_own.wait_recv()
    own_out[...] = part[0] + ddr[0]

    opp = []
    for i, h in enumerate(halves):
        x_f[i].wait_recv()
        opp.append(send(xb.at[2, 0, h], xb.at[2, 1, h], mate))
        y_f[i].wait_recv()
        opp.append(send(yb.at[2, 0, h], yb.at[2, 1, h], mate))
    m_f.wait_recv()
    opp.append(send(mb.at[2, 0], mb.at[2, 1], mate))
    place(1, 0)
    for c in opp:
        c.wait_recv()
    place(1, 1)
    experts(1, 0, n_loc)

    d_opp, hops = [], []

    def hop(n):
        cols = chunks[n]
        d_opp[n].wait_recv()
        osum[:, cols] = part[2, :, cols] + ddr[1, :, cols]
        hops.append((
            send(osum.at[pl.ds(0, half), cols], hopr.at[0, :, cols], right),
            send(osum.at[pl.ds(half, half), cols], hopr.at[1, :, cols], left)))

    for n, cols in enumerate(chunks):
        back(1, cols)
        combine(1, 1, cols)
        d_opp.append(send(part.at[3, :, cols], ddr.at[1, :, cols], mate))
        combine(1, 0, cols)
        if n >= LAG:
            hop(n - LAG)
    y_r.wait_recv()
    y_r2 = send(yb.at[3, 0], yb.at[3, 1], mate)
    x_l.wait_recv()
    x_l2 = send(xb.at[1, 0], xb.at[1, 1], mate)
    for n in range(n_cols - LAG, n_cols):
        hop(n)
    place(2, 0)
    place(2, 2)
    for c in early:
        c.wait_recv()
    y_r2.wait_recv()
    x_l2.wait_recv()
    place(2, 1)
    place(2, 3)
    experts(2, 0, n_loc)

    d_side = []

    def side(n):
        cols = chunks[n]
        for c in d_side[n]:
            c.wait_recv()
        for c in hops[n]:
            c.wait_recv()
        near, far = pl.ds(0, half), pl.ds(half, half)
        right_out[near, cols] = part[4, near, cols] + ddr[2, near, cols] + hopr[0, :, cols]
        right_out[far, cols] = part[4, far, cols] + ddr[2, far, cols]
        left_out[near, cols] = part[6, near, cols] + ddr[3, near, cols]
        left_out[far, cols] = part[6, far, cols] + ddr[3, far, cols] + hopr[1, :, cols]

    for n, cols in enumerate(chunks):
        back(2, cols)
        combine(2, 1, cols)
        combine(2, 3, cols)
        d_side.append((
            send(part.at[5, :, cols], ddr.at[2, :, cols], mate),
            send(part.at[7, :, cols], ddr.at[3, :, cols], mate)))
        combine(2, 0, cols)
        combine(2, 2, cols)
        if n >= LAG:
            side(n - LAG)
    for n in range(n_cols - LAG, n_cols):
        side(n)
    for c in made:
        c.wait_send()


def route(n_dev, cap, x, y, ids, slots, gates, w1, w2, w3):
    n_loc, d_model, d_ff = w1.shape
    top_k, tok = ids.shape
    n_rows = n_dev * cap
    hbm = pl.BlockSpec(memory_space=pltpu.HBM)
    vmem = pl.BlockSpec(memory_space=pltpu.VMEM)
    flops = 2 * n_loc * n_rows * d_model * d_ff * 5
    return pl.pallas_call(
        functools.partial(route_kernel, n_dev, cap),
        out_shape=(
            jax.ShapeDtypeStruct((n_loc, n_rows, d_model), BF),
            jax.ShapeDtypeStruct((n_loc, n_rows, d_model), BF),
            jax.ShapeDtypeStruct((n_loc, n_rows, d_ff), BF),
            jax.ShapeDtypeStruct((n_loc, n_rows, d_ff), BF),
            jax.ShapeDtypeStruct((n_loc, n_rows, d_ff), BF),
            jax.ShapeDtypeStruct((tok, d_model), F32),
            jax.ShapeDtypeStruct((tok, d_model), F32),
            jax.ShapeDtypeStruct((tok, d_model), F32),
        ),
        in_specs=[hbm] * 8,
        out_specs=[vmem] * 8,
        scratch_shapes=[
            pltpu.VMEM((4, 2, tok, d_model), BF),
            pltpu.VMEM((4, 2, tok, d_model), BF),
            pltpu.VMEM((4, 2, 2 * top_k, tok), F32),
            pltpu.VMEM(w1.shape, BF),
            pltpu.VMEM(w2.shape, BF),
            pltpu.VMEM(w3.shape, BF),
            pltpu.VMEM((n_loc, 4 * cap, d_model), BF),
            pltpu.VMEM((8, tok, n_loc * cap), BF),
            pltpu.VMEM((8, tok, d_model), F32),
            pltpu.VMEM((4, tok, d_model), F32),
            pltpu.VMEM((2, tok // 2, d_model), F32),
            pltpu.VMEM((tok, d_model), F32),
            pltpu.VMEM((top_k, tok), jnp.int32),
            pltpu.VMEM((top_k, tok), jnp.int32),
            pltpu.VMEM((top_k, tok), F32),
            pltpu.SemaphoreType.DMA((56,)),
            pltpu.SemaphoreType.DMA((56,)),
            pltpu.SemaphoreType.DMA((8,)),
        ],
        compiler_params=pltpu.CompilerParams(
            collective_id=0, has_side_effects=True, vmem_limit_bytes=36 * 1024 * 1024),
        cost_estimate=pl.CostEstimate(flops=flops, bytes_accessed=14 * 1024 * 1024, transcendentals=0),
        name="route",
    )(*(pltpu.with_memory_space_constraint(v, pltpu.HBM) for v in (x, y, ids, slots, gates, w1, w2, w3)))


def grad_kernel(x_ref, z_ref, h_ref, da_ref, db_ref, g1_ref, g2_ref, g3_ref):
    x = x_ref[0]
    g1_ref[0] = dot(x, da_ref[0], 0, 0)
    g3_ref[0] = dot(x, db_ref[0], 0, 0)
    g2_ref[0] = dot(h_ref[0], z_ref[0], 0, 0)


def grads(xr, zr, h, da, db, parts=2):
    n_loc, n_rows, d_model = xr.shape
    d_ff = h.shape[2]
    bm, bf = d_model // parts, d_ff // parts
    full = lambda width: pl.BlockSpec((1, n_rows, width), lambda e, i: (e, 0, 0))
    part = lambda width: pl.BlockSpec((1, n_rows, width), lambda e, i: (e, 0, i))
    return pl.pallas_call(
        grad_kernel,
        grid=(n_loc, parts),
        in_specs=[part(bm), full(d_model), part(bf), full(d_ff), full(d_ff)],
        out_specs=[
            pl.BlockSpec((1, bm, d_ff), lambda e, i: (e, i, 0)),
            pl.BlockSpec((1, bf, d_model), lambda e, i: (e, i, 0)),
            pl.BlockSpec((1, bm, d_ff), lambda e, i: (e, i, 0)),
        ],
        out_shape=(
            jax.ShapeDtypeStruct((n_loc, d_model, d_ff), F32),
            jax.ShapeDtypeStruct((n_loc, d_ff, d_model), F32),
            jax.ShapeDtypeStruct((n_loc, d_model, d_ff), F32),
        ),
        compiler_params=pltpu.CompilerParams(
            dimension_semantics=("arbitrary", "arbitrary"), vmem_limit_bytes=20 * 1024 * 1024),
        cost_estimate=pl.CostEstimate(
            flops=6 * n_loc * n_rows * d_model * d_ff, bytes_accessed=26 * 1024 * 1024, transcendentals=0),
        name="grads",
    )(xr, zr, h, da, db)


def solution(mesh):
    n_dev = mesh.shape["ep"]
    n_chip = n_dev // 2
    to_right = [(i, ((i // 2 + 1) % n_chip) * 2 + i % 2) for i in range(n_dev)]
    to_left = [(j, i) for i, j in to_right]

    def local_step(x_loc, dy_loc, ids_loc, gate_loc, slot_loc, w_gate, w_down, w_up):
        tok_dev, top_k = ids_loc.shape
        n_exp = w_gate.shape[0] * n_dev
        cap = slot_capacity(tok_dev, top_k, n_exp)
        xr, zr, h, da, db, own, right, left = route(
            n_dev, cap, x_loc, dy_loc, ids_loc.T, slot_loc.T, gate_loc.T, w_gate, w_down, w_up)
        from_left = lax.ppermute(right, "ep", to_right)
        from_right = lax.ppermute(left, "ep", to_left)
        g_gate, g_down, g_up = grads(xr, zr, h, da, db)
        dx = (own + from_left + from_right).astype(BF)
        return dx, g_gate, g_down, g_up

    tok_spec = P(("dp", "ep"), None)
    w_spec = P("ep", None, None)
    grad_spec = P(("dp", "ep"), None, None)
    return jax.shard_map(
        local_step, mesh=mesh,
        in_specs=(tok_spec, tok_spec, tok_spec, tok_spec, tok_spec, w_spec, w_spec, w_spec),
        out_specs=(tok_spec, grad_spec, grad_spec, grad_spec), check_vma=False)
```

```python
import functools

import jax
import jax.numpy as jnp
from jax import lax
from jax.experimental import pallas as pl
from jax.experimental.pallas import tpu as pltpu
from jax.sharding import PartitionSpec as P

BF = jnp.bfloat16
F32 = jnp.float32
COLS = 256


def slot_capacity(tok_dev, top_k, n_exp):
    return ((3 * tok_dev * top_k) // (2 * n_exp) + 7) // 8 * 8


def dot(a, b, ca=1, cb=0):
    return lax.dot_general(a, b, (((ca,), (cb,)), ((), ())), preferred_element_type=F32)


PASSES = (((0, 0), (0, 1)), ((2, 0), (2, 1)), ((1, 0), (1, 1), (3, 0), (3, 1)))
FIRST = (0, 2, 4)
LAG = 2


def route_kernel(
    n_dev, cap, x_hbm, y_hbm, ids_hbm, slots_hbm, gates_hbm, w1_hbm, w2_hbm, w3_hbm,
    xr, zr, hb, dab, dbb, own_out, right_out, left_out,
    xb, yb, mb, w1, w2, w3, w1t, w2t, w3t, dxb, oht, part, ddr, hopr, osum, ids, slots, gates,
    send_sem, recv_sem, load_sem,
):
    n_chip = n_dev // 2
    me = lax.axis_index("ep")
    chip, core = me // 2, me % 2
    right = {"ep": ((chip + 1) % n_chip) * 2 + core}
    left = {"ep": ((chip + n_chip - 1) % n_chip) * 2 + core}
    mate = {"ep": chip * 2 + 1 - core}
    n_loc, d_model, d_ff = w1.shape
    top_k, tok = ids.shape
    half = tok // 2
    halves = (pl.ds(0, half), pl.ds(half, half))

    loads = [
        pltpu.make_async_copy(src, dst, load_sem.at[i])
        for i, (src, dst) in enumerate((
            (x_hbm, xb.at[0, 0]), (y_hbm, yb.at[0, 0]), (ids_hbm, ids), (slots_hbm, slots), (gates_hbm, gates),
            (w2_hbm, w2), (w1_hbm, w1), (w3_hbm, w3)))
    ]
    for c in loads[:5]:
        c.start()

    barrier = pltpu.get_barrier_semaphore()
    for peer in (right, left, mate):
        pl.semaphore_signal(barrier, inc=1, device_id=peer, device_id_type=pl.DeviceIdType.MESH)

    for c in loads[2:5]:
        c.wait()
    mb[0, 0, 0:top_k, :] = jnp.where(slots[...] >= 0, ids[...] * cap + slots[...], -1).astype(F32)
    mb[0, 0, top_k:2 * top_k, :] = gates[...]

    for c in loads[:2]:
        c.wait()
    for c in loads[5:]:
        c.start()
    pl.semaphore_wait(barrier, 3)

    made = []

    def send(src, dst, peer):
        n = len(made)
        c = pltpu.make_async_remote_copy(
            src_ref=src, dst_ref=dst, send_sem=send_sem.at[n], recv_sem=recv_sem.at[n],
            device_id=peer, device_id_type=pl.DeviceIdType.MESH)
        c.start()
        made.append(c)
        return c

    x_r, y_l = [], []
    for h in halves:
        x_r.append(send(xb.at[0, 0, h], xb.at[3, 0, h], right))
        y_l.append(send(yb.at[0, 0, h], yb.at[1, 0, h], left))
    x_m = send(xb.at[0, 0], xb.at[0, 1], mate)
    m_m = send(mb.at[0, 0], mb.at[0, 1], mate)
    y_m = send(yb.at[0, 0], yb.at[0, 1], mate)
    m_r = send(mb.at[0, 0], mb.at[3, 0], right)
    m_l = send(mb.at[0, 0], mb.at[1, 0], left)

    row_id = lax.broadcasted_iota(jnp.int32, (n_loc * cap, tok), 0) + me * (n_loc * cap)

    def place(p, i):
        d, k = PASSES[p][i]
        q = FIRST[p] + i
        keys = mb[d, k, 0:top_k, :].astype(jnp.int32)
        gate_of = mb[d, k, top_k:2 * top_k, :]
        hot = jnp.zeros((n_loc * cap, tok), F32)
        gate = jnp.zeros((n_loc * cap, tok), F32)
        for j in range(top_k):
            hit = keys[j:j + 1, :] == row_id
            hot = jnp.where(hit, 1.0, hot)
            gate = jnp.where(hit, gate_of[j:j + 1, :], gate)
        gate_row = jnp.sum(gate, axis=1, keepdims=True)
        hot = hot.astype(BF)
        oht[q] = hot.T
        for n in range(d_model // COLS):
            cols = pl.ds(n * COLS, COLS)
            xv = dot(hot, xb[d, k, :, cols]).astype(BF)
            zv = (dot(hot, yb[d, k, :, cols]) * gate_row).astype(BF)
            for e in range(n_loc):
                xr[e, pl.ds(q * cap, cap), cols] = xv[e * cap:(e + 1) * cap]
                zr[e, pl.ds(q * cap, cap), cols] = zv[e * cap:(e + 1) * cap]

    def turn(src, dst):
        def one(e, carry):
            for n in range(src.shape[1] // COLS):
                cols = pl.ds(n * COLS, COLS)
                dst[e, :, cols] = src[e, cols, :].T
            return carry

        lax.fori_loop(0, n_loc, one, 0)

    def inner(p, e):
        at = pl.ds(FIRST[p] * cap, len(PASSES[p]) * cap)
        x_e = xr[e, at, :]
        z_e = zr[e, at, :]
        for n in range(d_ff // COLS):
            cols = pl.ds(n * COLS, COLS)
            a = dot(x_e, w1[e, :, cols]).astype(BF).astype(F32)
            b = dot(x_e, w3[e, :, cols]).astype(BF).astype(F32)
            dh = dot(z_e, w2t[e, :, cols])
            sg = jax.nn.sigmoid(a)
            act = a * sg
            hb[e, at, cols] = (act * b).astype(BF)
            dab[e, at, cols] = (dh * b * sg * (1.0 + a * (1.0 - sg))).astype(BF)
            dbb[e, at, cols] = (dh * act).astype(BF)

    def experts(p, lo, hi):
        lax.fori_loop(lo, hi, lambda e, c: (inner(p, e), c)[1], 0)

    def back(p, cols):
        rows = len(PASSES[p]) * cap
        at = pl.ds(FIRST[p] * cap, rows)

        def one(e, carry):
            dxb[e, pl.ds(0, rows), cols] = (
                dot(dab[e, at, :], w1t[e, :, cols]) + dot(dbb[e, at, :], w3t[e, :, cols])).astype(BF)
            return carry

        for e in range(n_loc):
            one(e, 0)

    def combine(p, i, cols):
        q = FIRST[p] + i
        rows = jnp.concatenate([dxb[e, pl.ds(i * cap, cap), cols] for e in range(n_loc)], axis=0)
        part[q, :, cols] = dot(oht[q], rows)

    def forward(i):
        x_r[i].wait_recv()
        x_f.append(send(xb.at[3, 0, halves[i]], xb.at[2, 0, halves[i]], right))
        y_l[i].wait_recv()
        y_f.append(send(yb.at[1, 0, halves[i]], yb.at[2, 0, halves[i]], left))

    n_cols = d_model // COLS
    chunks = [pl.ds(n * COLS, COLS) for n in range(n_cols)]
    x_f, y_f = [], []
    place(0, 0)
    loads[5].wait()
    turn(w2, w2t)
    m_m.wait_recv()
    x_m.wait_recv()
    y_m.wait_recv()
    place(0, 1)
    forward(0)
    loads[6].wait()
    turn(w1, w1t)
    loads[7].wait()
    turn(w3, w3t)
    forward(1)
    m_r.wait_recv()
    m_f = send(mb.at[3, 0], mb.at[2, 0], right)
    y_r = send(yb.at[0, 0], yb.at[3, 0], right)
    x_l = send(xb.at[0, 0], xb.at[1, 0], left)
    m_l.wait_recv()
    early = [
        send(mb.at[3, 0], mb.at[3, 1], mate),
        send(mb.at[1, 0], mb.at[1, 1], mate),
        send(xb.at[3, 0], xb.at[3, 1], mate),
        send(yb.at[1, 0], yb.at[1, 1], mate),
    ]
    experts(0, 0, n_loc)
    for cols in chunks:
        back(0, cols)
        combine(0, 1, cols)
    d_own = send(part.at[1], ddr.at[0], mate)
    for cols in chunks:
        combine(0, 0, cols)
    d_own.wait_recv()
    own_out[...] = part[0] + ddr[0]

    opp = []
    for i, h in enumerate(halves):
        x_f[i].wait_recv()
        opp.append(send(xb.at[2, 0, h], xb.at[2, 1, h], mate))
        y_f[i].wait_recv()
        opp.append(send(yb.at[2, 0, h], yb.at[2, 1, h], mate))
    m_f.wait_recv()
    opp.append(send(mb.at[2, 0], mb.at[2, 1], mate))
    place(1, 0)
    for c in opp:
        c.wait_recv()
    place(1, 1)
    experts(1, 0, n_loc)

    d_opp, hops = [], []

    def hop(n):
        cols = chunks[n]
        d_opp[n].wait_recv()
        osum[:, cols] = part[2, :, cols] + ddr[1, :, cols]
        hops.append((
            send(osum.at[pl.ds(0, half), cols], hopr.at[0, :, cols], right),
            send(osum.at[pl.ds(half, half), cols], hopr.at[1, :, cols], left)))

    for n, cols in enumerate(chunks):
        back(1, cols)
        combine(1, 1, cols)
        d_opp.append(send(part.at[3, :, cols], ddr.at[1, :, cols], mate))
        combine(1, 0, cols)
        if n >= LAG:
            hop(n - LAG)
    y_r.wait_recv()
    y_r2 = send(yb.at[3, 0], yb.at[3, 1], mate)
    x_l.wait_recv()
    x_l2 = send(xb.at[1, 0], xb.at[1, 1], mate)
    for n in range(n_cols - LAG, n_cols):
        hop(n)
    place(2, 0)
    place(2, 2)
    for c in early:
        c.wait_recv()
    y_r2.wait_recv()
    x_l2.wait_recv()
    place(2, 1)
    place(2, 3)
    experts(2, 0, n_loc)

    d_side = []

    def side(n):
        cols = chunks[n]
        for c in d_side[n]:
            c.wait_recv()
        for c in hops[n]:
            c.wait_recv()
        near, far = pl.ds(0, half), pl.ds(half, half)
        right_out[near, cols] = part[4, near, cols] + ddr[2, near, cols] + hopr[0, :, cols]
        right_out[far, cols] = part[4, far, cols] + ddr[2, far, cols]
        left_out[near, cols] = part[6, near, cols] + ddr[3, near, cols]
        left_out[far, cols] = part[6, far, cols] + ddr[3, far, cols] + hopr[1, :, cols]

    for n, cols in enumerate(chunks):
        back(2, cols)
        combine(2, 1, cols)
        combine(2, 3, cols)
        d_side.append((
            send(part.at[5, :, cols], ddr.at[2, :, cols], mate),
            send(part.at[7, :, cols], ddr.at[3, :, cols], mate)))
        combine(2, 0, cols)
        combine(2, 2, cols)
        if n >= LAG:
            side(n - LAG)
    for n in range(n_cols - LAG, n_cols):
        side(n)
    for c in made:
        c.wait_send()


def route(n_dev, cap, x, y, ids, slots, gates, w1, w2, w3):
    n_loc, d_model, d_ff = w1.shape
    top_k, tok = ids.shape
    n_rows = n_dev * cap
    hbm = pl.BlockSpec(memory_space=pltpu.HBM)
    vmem = pl.BlockSpec(memory_space=pltpu.VMEM)
    flops = 2 * n_loc * n_rows * d_model * d_ff * 5
    return pl.pallas_call(
        functools.partial(route_kernel, n_dev, cap),
        out_shape=(
            jax.ShapeDtypeStruct((n_loc, n_rows, d_model), BF),
            jax.ShapeDtypeStruct((n_loc, n_rows, d_model), BF),
            jax.ShapeDtypeStruct((n_loc, n_rows, d_ff), BF),
            jax.ShapeDtypeStruct((n_loc, n_rows, d_ff), BF),
            jax.ShapeDtypeStruct((n_loc, n_rows, d_ff), BF),
            jax.ShapeDtypeStruct((tok, d_model), F32),
            jax.ShapeDtypeStruct((tok, d_model), F32),
            jax.ShapeDtypeStruct((tok, d_model), F32),
        ),
        in_specs=[hbm] * 8,
        out_specs=[vmem] * 8,
        scratch_shapes=[
            pltpu.VMEM((4, 2, tok, d_model), BF),
            pltpu.VMEM((4, 2, tok, d_model), BF),
            pltpu.VMEM((4, 2, 2 * top_k, tok), F32),
            pltpu.VMEM(w1.shape, BF),
            pltpu.VMEM(w2.shape, BF),
            pltpu.VMEM(w3.shape, BF),
            pltpu.VMEM(w2.shape, BF),
            pltpu.VMEM(w1.shape, BF),
            pltpu.VMEM(w2.shape, BF),
            pltpu.VMEM((n_loc, 4 * cap, d_model), BF),
            pltpu.VMEM((8, tok, n_loc * cap), BF),
            pltpu.VMEM((8, tok, d_model), F32),
            pltpu.VMEM((4, tok, d_model), F32),
            pltpu.VMEM((2, tok // 2, d_model), F32),
            pltpu.VMEM((tok, d_model), F32),
            pltpu.VMEM((top_k, tok), jnp.int32),
            pltpu.VMEM((top_k, tok), jnp.int32),
            pltpu.VMEM((top_k, tok), F32),
            pltpu.SemaphoreType.DMA((56,)),
            pltpu.SemaphoreType.DMA((56,)),
            pltpu.SemaphoreType.DMA((8,)),
        ],
        compiler_params=pltpu.CompilerParams(
            collective_id=0, has_side_effects=True, vmem_limit_bytes=41 * 1024 * 1024),
        cost_estimate=pl.CostEstimate(flops=flops, bytes_accessed=14 * 1024 * 1024, transcendentals=0),
        name="route",
    )(*(pltpu.with_memory_space_constraint(v, pltpu.HBM) for v in (x, y, ids, slots, gates, w1, w2, w3)))


def grad_kernel(x_ref, z_ref, h_ref, da_ref, db_ref, g1_ref, g2_ref, g3_ref):
    x = x_ref[0]
    g1_ref[0] = dot(x, da_ref[0], 0, 0)
    g3_ref[0] = dot(x, db_ref[0], 0, 0)
    g2_ref[0] = dot(h_ref[0], z_ref[0], 0, 0)


def grads(xr, zr, h, da, db, parts=2):
    n_loc, n_rows, d_model = xr.shape
    d_ff = h.shape[2]
    bm, bf = d_model // parts, d_ff // parts
    full = lambda width: pl.BlockSpec((1, n_rows, width), lambda e, i: (e, 0, 0))
    part = lambda width: pl.BlockSpec((1, n_rows, width), lambda e, i: (e, 0, i))
    return pl.pallas_call(
        grad_kernel,
        grid=(n_loc, parts),
        in_specs=[part(bm), full(d_model), part(bf), full(d_ff), full(d_ff)],
        out_specs=[
            pl.BlockSpec((1, bm, d_ff), lambda e, i: (e, i, 0)),
            pl.BlockSpec((1, bf, d_model), lambda e, i: (e, i, 0)),
            pl.BlockSpec((1, bm, d_ff), lambda e, i: (e, i, 0)),
        ],
        out_shape=(
            jax.ShapeDtypeStruct((n_loc, d_model, d_ff), F32),
            jax.ShapeDtypeStruct((n_loc, d_ff, d_model), F32),
            jax.ShapeDtypeStruct((n_loc, d_model, d_ff), F32),
        ),
        compiler_params=pltpu.CompilerParams(
            dimension_semantics=("arbitrary", "arbitrary"), vmem_limit_bytes=20 * 1024 * 1024),
        cost_estimate=pl.CostEstimate(
            flops=6 * n_loc * n_rows * d_model * d_ff, bytes_accessed=26 * 1024 * 1024, transcendentals=0),
        name="grads",
    )(xr, zr, h, da, db)


def solution(mesh):
    n_dev = mesh.shape["ep"]
    n_chip = n_dev // 2
    to_right = [(i, ((i // 2 + 1) % n_chip) * 2 + i % 2) for i in range(n_dev)]
    to_left = [(j, i) for i, j in to_right]

    def local_step(x_loc, dy_loc, ids_loc, gate_loc, slot_loc, w_gate, w_down, w_up):
        tok_dev, top_k = ids_loc.shape
        n_exp = w_gate.shape[0] * n_dev
        cap = slot_capacity(tok_dev, top_k, n_exp)
        xr, zr, h, da, db, own, right, left = route(
            n_dev, cap, x_loc, dy_loc, ids_loc.T, slot_loc.T, gate_loc.T, w_gate, w_down, w_up)
        from_left = lax.ppermute(right, "ep", to_right)
        from_right = lax.ppermute(left, "ep", to_left)
        g_gate, g_down, g_up = grads(xr, zr, h, da, db)
        dx = (own + from_left + from_right).astype(BF)
        return dx, g_gate, g_down, g_up

    tok_spec = P(("dp", "ep"), None)
    w_spec = P("ep", None, None)
    grad_spec = P(("dp", "ep"), None, None)
    return jax.shard_map(
        local_step, mesh=mesh,
        in_specs=(tok_spec, tok_spec, tok_spec, tok_spec, tok_spec, w_spec, w_spec, w_spec),
        out_specs=(tok_spec, grad_spec, grad_spec, grad_spec), check_vma=False)
```

```python
import functools

import jax
import jax.numpy as jnp
from jax import lax
from jax.experimental import pallas as pl
from jax.experimental.pallas import tpu as pltpu
from jax.sharding import PartitionSpec as P

BF = jnp.bfloat16
F32 = jnp.float32
COLS = 256


def slot_capacity(tok_dev, top_k, n_exp):
    return ((3 * tok_dev * top_k) // (2 * n_exp) + 7) // 8 * 8


def dot(a, b, ca=1, cb=0):
    return lax.dot_general(a, b, (((ca,), (cb,)), ((), ())), preferred_element_type=F32)


PASSES = (((0, 0), (0, 1)), ((2, 0), (2, 1)), ((1, 0), (1, 1), (3, 0), (3, 1)))
FIRST = (0, 2, 4)
LAG = 2


def route_kernel(
    n_dev, cap, x_hbm, y_hbm, ids_hbm, slots_hbm, gates_hbm, w1_hbm, w2_hbm, w3_hbm,
    xr, zr, hb, dab, dbb, own_out, right_out, left_out,
    xb, yb, mb, w1, w2, w3, w1t, w2t, w3t, dxb, oh, oht, gr, part, ddr, hopr, osum, ids, slots, gates,
    send_sem, recv_sem, load_sem,
):
    n_chip = n_dev // 2
    me = lax.axis_index("ep")
    chip, core = me // 2, me % 2
    right = {"ep": ((chip + 1) % n_chip) * 2 + core}
    left = {"ep": ((chip + n_chip - 1) % n_chip) * 2 + core}
    mate = {"ep": chip * 2 + 1 - core}
    n_loc, d_model, d_ff = w1.shape
    top_k, tok = ids.shape
    half = tok // 2
    halves = (pl.ds(0, half), pl.ds(half, half))

    loads = [
        pltpu.make_async_copy(src, dst, load_sem.at[i])
        for i, (src, dst) in enumerate((
            (x_hbm, xb.at[0, 0]), (y_hbm, yb.at[0, 0]), (ids_hbm, ids), (slots_hbm, slots), (gates_hbm, gates),
            (w2_hbm, w2), (w1_hbm, w1), (w3_hbm, w3)))
    ]
    for c in loads[:5]:
        c.start()

    barrier = pltpu.get_barrier_semaphore()
    for peer in (right, left, mate):
        pl.semaphore_signal(barrier, inc=1, device_id=peer, device_id_type=pl.DeviceIdType.MESH)

    for c in loads[2:5]:
        c.wait()
    mb[0, 0, 0:top_k, :] = jnp.where(slots[...] >= 0, ids[...] * cap + slots[...], -1).astype(F32)
    mb[0, 0, top_k:2 * top_k, :] = gates[...]

    for c in loads[:2]:
        c.wait()
    for c in loads[5:]:
        c.start()
    pl.semaphore_wait(barrier, 3)

    made = []

    def send(src, dst, peer):
        n = len(made)
        c = pltpu.make_async_remote_copy(
            src_ref=src, dst_ref=dst, send_sem=send_sem.at[n], recv_sem=recv_sem.at[n],
            device_id=peer, device_id_type=pl.DeviceIdType.MESH)
        c.start()
        made.append(c)
        return c

    x_r, y_l = [], []
    for h in halves:
        x_r.append(send(xb.at[0, 0, h], xb.at[3, 0, h], right))
        y_l.append(send(yb.at[0, 0, h], yb.at[1, 0, h], left))
    x_m = send(xb.at[0, 0], xb.at[0, 1], mate)
    m_m = send(mb.at[0, 0], mb.at[0, 1], mate)
    y_m = send(yb.at[0, 0], yb.at[0, 1], mate)
    m_r = send(mb.at[0, 0], mb.at[3, 0], right)
    m_l = send(mb.at[0, 0], mb.at[1, 0], left)

    row_id = lax.broadcasted_iota(jnp.int32, (n_loc * cap, tok), 0) + me * (n_loc * cap)

    def mask(p, i):
        d, k = PASSES[p][i]
        q = FIRST[p] + i
        keys = mb[d, k, 0:top_k, :].astype(jnp.int32)
        gate_of = mb[d, k, top_k:2 * top_k, :]
        hot = jnp.zeros((n_loc * cap, tok), F32)
        gate = jnp.zeros((n_loc * cap, tok), F32)
        for j in range(top_k):
            hit = keys[j:j + 1, :] == row_id
            hot = jnp.where(hit, 1.0, hot)
            gate = jnp.where(hit, gate_of[j:j + 1, :], gate)
        hot = hot.astype(BF)
        oh[q] = hot
        oht[q] = hot.T
        gr[q] = jnp.broadcast_to(jnp.sum(gate, axis=1, keepdims=True), gate.shape)

    def place_x(p, i):
        d, k = PASSES[p][i]
        q = FIRST[p] + i
        hot = oh[q]
        for n in range(d_model // COLS):
            cols = pl.ds(n * COLS, COLS)
            xv = dot(hot, xb[d, k, :, cols]).astype(BF)
            for e in range(n_loc):
                xr[e, pl.ds(q * cap, cap), cols] = xv[e * cap:(e + 1) * cap]

    def place_z(p, i):
        d, k = PASSES[p][i]
        q = FIRST[p] + i
        hot = oh[q]
        gate_row = jnp.concatenate([gr[q]] * (COLS // tok), axis=1)
        for n in range(d_model // COLS):
            cols = pl.ds(n * COLS, COLS)
            zv = (dot(hot, yb[d, k, :, cols]) * gate_row).astype(BF)
            for e in range(n_loc):
                zr[e, pl.ds(q * cap, cap), cols] = zv[e * cap:(e + 1) * cap]

    def place(p, i):
        place_x(p, i)
        place_z(p, i)

    def turn(src, dst):
        def one(e, carry):
            for n in range(src.shape[1] // COLS):
                cols = pl.ds(n * COLS, COLS)
                dst[e, :, cols] = src[e, cols, :].T
            return carry

        lax.fori_loop(0, n_loc, one, 0)

    def inner(p, e):
        at = pl.ds(FIRST[p] * cap, len(PASSES[p]) * cap)
        x_e = xr[e, at, :]
        z_e = zr[e, at, :]
        for n in range(d_ff // COLS):
            cols = pl.ds(n * COLS, COLS)
            a = dot(x_e, w1[e, :, cols]).astype(BF).astype(F32)
            b = dot(x_e, w3[e, :, cols]).astype(BF).astype(F32)
            dh = dot(z_e, w2t[e, :, cols])
            sg = jax.nn.sigmoid(a)
            act = a * sg
            hb[e, at, cols] = (act * b).astype(BF)
            dab[e, at, cols] = (dh * b * sg * (1.0 + a * (1.0 - sg))).astype(BF)
            dbb[e, at, cols] = (dh * act).astype(BF)

    def experts(p, lo, hi):
        lax.fori_loop(lo, hi, lambda e, c: (inner(p, e), c)[1], 0)

    def back(p, cols):
        rows = len(PASSES[p]) * cap
        at = pl.ds(FIRST[p] * cap, rows)

        def one(e, carry):
            dxb[e, pl.ds(0, rows), cols] = (
                dot(dab[e, at, :], w1t[e, :, cols]) + dot(dbb[e, at, :], w3t[e, :, cols])).astype(BF)
            return carry

        for e in range(n_loc):
            one(e, 0)

    sums = (own_out, part.at[0], osum, part.at[1], right_out, part.at[2], left_out, part.at[3])

    def combine(p, i, cols):
        q = FIRST[p] + i
        rows = jnp.concatenate([dxb[e, pl.ds(i * cap, cap), cols] for e in range(n_loc)], axis=0)
        sums[q][:, cols] = dot(oht[q], rows)

    def forward(i):
        x_r[i].wait_recv()
        x_f.append(send(xb.at[3, 0, halves[i]], xb.at[2, 0, halves[i]], right))
        y_l[i].wait_recv()
        y_f.append(send(yb.at[1, 0, halves[i]], yb.at[2, 0, halves[i]], left))

    n_cols = d_model // COLS
    chunks = [pl.ds(n * COLS, COLS) for n in range(n_cols)]
    x_f, y_f = [], []
    mask(0, 0)
    place(0, 0)
    loads[5].wait()
    turn(w2, w2t)
    m_m.wait_recv()
    mask(0, 1)
    x_m.wait_recv()
    y_m.wait_recv()
    place(0, 1)
    forward(0)
    loads[6].wait()
    turn(w1, w1t)
    loads[7].wait()
    turn(w3, w3t)
    forward(1)
    m_r.wait_recv()
    m_f = send(mb.at[3, 0], mb.at[2, 0], right)
    y_r = send(yb.at[0, 0], yb.at[3, 0], right)
    x_l = send(xb.at[0, 0], xb.at[1, 0], left)
    m_l.wait_recv()
    early = [
        send(mb.at[3, 0], mb.at[3, 1], mate),
        send(mb.at[1, 0], mb.at[1, 1], mate),
        send(xb.at[3, 0], xb.at[3, 1], mate),
        send(yb.at[1, 0], yb.at[1, 1], mate),
    ]
    experts(0, 0, n_loc)
    for cols in chunks:
        back(0, cols)
        combine(0, 1, cols)
    d_own = send(sums[1], ddr.at[0], mate)
    for cols in chunks:
        combine(0, 0, cols)
    d_own.wait_recv()
    own_out[...] += ddr[0]
    for i in range(2):
        early[i].wait_recv()
    for i in range(4):
        mask(2, i)
    place_z(2, 0)
    place_x(2, 2)
    m_f.wait_recv()
    m_f2 = send(mb.at[2, 0], mb.at[2, 1], mate)
    mask(1, 0)

    opp = []
    for i, h in enumerate(halves):
        x_f[i].wait_recv()
        opp.append(send(xb.at[2, 0, h], xb.at[2, 1, h], mate))
        y_f[i].wait_recv()
        opp.append(send(yb.at[2, 0, h], yb.at[2, 1, h], mate))
    m_f2.wait_recv()
    mask(1, 1)
    place(1, 0)
    for c in opp:
        c.wait_recv()
    place(1, 1)
    experts(1, 0, n_loc)

    d_opp, hops = [], []

    def hop(n):
        cols = chunks[n]
        d_opp[n].wait_recv()
        osum[:, cols] += ddr[1, :, cols]
        hops.append((
            send(osum.at[pl.ds(0, half), cols], hopr.at[0, :, cols], right),
            send(osum.at[pl.ds(half, half), cols], hopr.at[1, :, cols], left)))

    for n, cols in enumerate(chunks):
        back(1, cols)
        combine(1, 1, cols)
        d_opp.append(send(sums[3].at[:, cols], ddr.at[1, :, cols], mate))
        combine(1, 0, cols)
        if n >= LAG:
            hop(n - LAG)
    y_r.wait_recv()
    y_r2 = send(yb.at[3, 0], yb.at[3, 1], mate)
    x_l.wait_recv()
    x_l2 = send(xb.at[1, 0], xb.at[1, 1], mate)
    for n in range(n_cols - LAG, n_cols):
        hop(n)
    for c in early[2:]:
        c.wait_recv()
    place_z(2, 1)
    place_x(2, 3)
    place_x(2, 0)
    place_z(2, 2)
    y_r2.wait_recv()
    x_l2.wait_recv()
    place_x(2, 1)
    place_z(2, 3)
    experts(2, 0, n_loc)

    d_side = []

    def side(n):
        cols = chunks[n]
        for c in d_side[n]:
            c.wait_recv()
        for c in hops[n]:
            c.wait_recv()
        near, far = pl.ds(0, half), pl.ds(half, half)
        right_out[near, cols] += ddr[2, near, cols] + hopr[0, :, cols]
        right_out[far, cols] += ddr[2, far, cols]
        left_out[near, cols] += ddr[3, near, cols]
        left_out[far, cols] += ddr[3, far, cols] + hopr[1, :, cols]

    for n, cols in enumerate(chunks):
        back(2, cols)
        combine(2, 1, cols)
        combine(2, 3, cols)
        d_side.append((
            send(sums[5].at[:, cols], ddr.at[2, :, cols], mate),
            send(sums[7].at[:, cols], ddr.at[3, :, cols], mate)))
        combine(2, 0, cols)
        combine(2, 2, cols)
        if n >= LAG:
            side(n - LAG)
    for n in range(n_cols - LAG, n_cols):
        side(n)
    for c in made:
        c.wait_send()


def route(n_dev, cap, x, y, ids, slots, gates, w1, w2, w3):
    n_loc, d_model, d_ff = w1.shape
    top_k, tok = ids.shape
    n_rows = n_dev * cap
    hbm = pl.BlockSpec(memory_space=pltpu.HBM)
    vmem = pl.BlockSpec(memory_space=pltpu.VMEM)
    flops = 2 * n_loc * n_rows * d_model * d_ff * 5
    return pl.pallas_call(
        functools.partial(route_kernel, n_dev, cap),
        out_shape=(
            jax.ShapeDtypeStruct((n_loc, n_rows, d_model), BF),
            jax.ShapeDtypeStruct((n_loc, n_rows, d_model), BF),
            jax.ShapeDtypeStruct((n_loc, n_rows, d_ff), BF),
            jax.ShapeDtypeStruct((n_loc, n_rows, d_ff), BF),
            jax.ShapeDtypeStruct((n_loc, n_rows, d_ff), BF),
            jax.ShapeDtypeStruct((tok, d_model), F32),
            jax.ShapeDtypeStruct((tok, d_model), F32),
            jax.ShapeDtypeStruct((tok, d_model), F32),
        ),
        in_specs=[hbm] * 8,
        out_specs=[vmem] * 8,
        scratch_shapes=[
            pltpu.VMEM((4, 2, tok, d_model), BF),
            pltpu.VMEM((4, 2, tok, d_model), BF),
            pltpu.VMEM((4, 2, 2 * top_k, tok), F32),
            pltpu.VMEM(w1.shape, BF),
            pltpu.VMEM(w2.shape, BF),
            pltpu.VMEM(w3.shape, BF),
            pltpu.VMEM(w2.shape, BF),
            pltpu.VMEM(w1.shape, BF),
            pltpu.VMEM(w2.shape, BF),
            pltpu.VMEM((n_loc, 4 * cap, d_model), BF),
            pltpu.VMEM((8, n_loc * cap, tok), BF),
            pltpu.VMEM((8, tok, n_loc * cap), BF),
            pltpu.VMEM((8, n_loc * cap, tok), F32),
            pltpu.VMEM((4, tok, d_model), F32),
            pltpu.VMEM((4, tok, d_model), F32),
            pltpu.VMEM((2, tok // 2, d_model), F32),
            pltpu.VMEM((tok, d_model), F32),
            pltpu.VMEM((top_k, tok), jnp.int32),
            pltpu.VMEM((top_k, tok), jnp.int32),
            pltpu.VMEM((top_k, tok), F32),
            pltpu.SemaphoreType.DMA((56,)),
            pltpu.SemaphoreType.DMA((56,)),
            pltpu.SemaphoreType.DMA((8,)),
        ],
        compiler_params=pltpu.CompilerParams(
            collective_id=0, has_side_effects=True, vmem_limit_bytes=42000000),
        cost_estimate=pl.CostEstimate(flops=flops, bytes_accessed=14 * 1024 * 1024, transcendentals=0),
        name="route",
    )(*(pltpu.with_memory_space_constraint(v, pltpu.HBM) for v in (x, y, ids, slots, gates, w1, w2, w3)))


def grad_kernel(x_ref, z_ref, h_ref, da_ref, db_ref, g1_ref, g2_ref, g3_ref):
    x = x_ref[0]
    g1_ref[0] = dot(x, da_ref[0], 0, 0)
    g3_ref[0] = dot(x, db_ref[0], 0, 0)
    g2_ref[0] = dot(h_ref[0], z_ref[0], 0, 0)


def grads(xr, zr, h, da, db, parts=2):
    n_loc, n_rows, d_model = xr.shape
    d_ff = h.shape[2]
    bm, bf = d_model // parts, d_ff // parts
    full = lambda width: pl.BlockSpec((1, n_rows, width), lambda e, i: (e, 0, 0))
    part = lambda width: pl.BlockSpec((1, n_rows, width), lambda e, i: (e, 0, i))
    return pl.pallas_call(
        grad_kernel,
        grid=(n_loc, parts),
        in_specs=[part(bm), full(d_model), part(bf), full(d_ff), full(d_ff)],
        out_specs=[
            pl.BlockSpec((1, bm, d_ff), lambda e, i: (e, i, 0)),
            pl.BlockSpec((1, bf, d_model), lambda e, i: (e, i, 0)),
            pl.BlockSpec((1, bm, d_ff), lambda e, i: (e, i, 0)),
        ],
        out_shape=(
            jax.ShapeDtypeStruct((n_loc, d_model, d_ff), F32),
            jax.ShapeDtypeStruct((n_loc, d_ff, d_model), F32),
            jax.ShapeDtypeStruct((n_loc, d_model, d_ff), F32),
        ),
        compiler_params=pltpu.CompilerParams(
            dimension_semantics=("arbitrary", "arbitrary"), vmem_limit_bytes=20 * 1024 * 1024),
        cost_estimate=pl.CostEstimate(
            flops=6 * n_loc * n_rows * d_model * d_ff, bytes_accessed=26 * 1024 * 1024, transcendentals=0),
        name="grads",
    )(xr, zr, h, da, db)


def solution(mesh):
    n_dev = mesh.shape["ep"]
    n_chip = n_dev // 2
    to_right = [(i, ((i // 2 + 1) % n_chip) * 2 + i % 2) for i in range(n_dev)]
    to_left = [(j, i) for i, j in to_right]

    def local_step(x_loc, dy_loc, ids_loc, gate_loc, slot_loc, w_gate, w_down, w_up):
        tok_dev, top_k = ids_loc.shape
        n_exp = w_gate.shape[0] * n_dev
        cap = slot_capacity(tok_dev, top_k, n_exp)
        xr, zr, h, da, db, own, right, left = route(
            n_dev, cap, x_loc, dy_loc, ids_loc.T, slot_loc.T, gate_loc.T, w_gate, w_down, w_up)
        from_left = lax.ppermute(right, "ep", to_right)
        from_right = lax.ppermute(left, "ep", to_left)
        g_gate, g_down, g_up = grads(xr, zr, h, da, db)
        dx = (own + from_left + from_right).astype(BF)
        return dx, g_gate, g_down, g_up

    tok_spec = P(("dp", "ep"), None)
    w_spec = P("ep", None, None)
    grad_spec = P(("dp", "ep"), None, None)
    return jax.shard_map(
        local_step, mesh=mesh,
        in_specs=(tok_spec, tok_spec, tok_spec, tok_spec, tok_spec, w_spec, w_spec, w_spec),
        out_specs=(tok_spec, grad_spec, grad_spec, grad_spec), check_vma=False)
```

```python
import functools

import jax
import jax.numpy as jnp
from jax import lax
from jax.experimental import pallas as pl
from jax.experimental.pallas import tpu as pltpu
from jax.sharding import PartitionSpec as P

BF = jnp.bfloat16
F32 = jnp.float32
COLS = 256


def slot_capacity(tok_dev, top_k, n_exp):
    return ((3 * tok_dev * top_k) // (2 * n_exp) + 7) // 8 * 8


def dot(a, b, ca=1, cb=0):
    return lax.dot_general(a, b, (((ca,), (cb,)), ((), ())), preferred_element_type=F32)


PASSES = (((0, 0), (0, 1)), ((2, 0), (2, 1)), ((1, 0), (1, 1), (3, 0), (3, 1)))
FIRST = (0, 2, 4)
LAG = 2


def route_kernel(
    n_dev, cap, x_hbm, y_hbm, ids_hbm, slots_hbm, gates_hbm, w1_hbm, w2_hbm, w3_hbm,
    xr, zr, hb, dab, dbb, own_out, right_out, left_out,
    xb, yb, mb, w1, w2, w3, w1t, w2t, w3t, dxb, oh, oht, gr, part, ddr, hopr, osum, ids, slots, gates,
    send_sem, recv_sem, load_sem,
):
    n_chip = n_dev // 2
    me = lax.axis_index("ep")
    chip, core = me // 2, me % 2
    right = {"ep": ((chip + 1) % n_chip) * 2 + core}
    left = {"ep": ((chip + n_chip - 1) % n_chip) * 2 + core}
    mate = {"ep": chip * 2 + 1 - core}
    n_loc, d_model, d_ff = w1.shape
    top_k, tok = ids.shape
    half = tok // 2
    halves = (pl.ds(0, half), pl.ds(half, half))

    loads = [
        pltpu.make_async_copy(src, dst, load_sem.at[i])
        for i, (src, dst) in enumerate((
            (x_hbm, xb.at[0, 0]), (y_hbm, yb.at[0, 0]), (ids_hbm, ids), (slots_hbm, slots), (gates_hbm, gates),
            (w2_hbm, w2), (w1_hbm, w1), (w3_hbm, w3)))
    ]
    for c in loads[:5]:
        c.start()

    barrier = pltpu.get_barrier_semaphore()
    for peer in (right, left, mate):
        pl.semaphore_signal(barrier, inc=1, device_id=peer, device_id_type=pl.DeviceIdType.MESH)

    for c in loads[2:5]:
        c.wait()
    mb[0, 0, 0:top_k, :] = jnp.where(slots[...] >= 0, ids[...] * cap + slots[...], -1).astype(F32)
    mb[0, 0, top_k:2 * top_k, :] = gates[...]

    for c in loads[:2]:
        c.wait()
    for c in loads[5:]:
        c.start()
    pl.semaphore_wait(barrier, 3)

    made = []

    def send(src, dst, peer):
        n = len(made)
        c = pltpu.make_async_remote_copy(
            src_ref=src, dst_ref=dst, send_sem=send_sem.at[n], recv_sem=recv_sem.at[n],
            device_id=peer, device_id_type=pl.DeviceIdType.MESH)
        c.start()
        made.append(c)
        return c

    x_r, y_l = [], []
    for h in halves:
        x_r.append(send(xb.at[0, 0, h], xb.at[3, 0, h], right))
        y_l.append(send(yb.at[0, 0, h], yb.at[1, 0, h], left))
    x_m = send(xb.at[0, 0], xb.at[0, 1], mate)
    m_m = send(mb.at[0, 0], mb.at[0, 1], mate)
    y_m = send(yb.at[0, 0], yb.at[0, 1], mate)
    m_r = send(mb.at[0, 0], mb.at[3, 0], right)
    m_l = send(mb.at[0, 0], mb.at[1, 0], left)

    row_id = lax.broadcasted_iota(jnp.int32, (n_loc * cap, tok), 0) + me * (n_loc * cap)

    def mask(p, i):
        d, k = PASSES[p][i]
        q = FIRST[p] + i
        keys = mb[d, k, 0:top_k, :].astype(jnp.int32)
        gate_of = mb[d, k, top_k:2 * top_k, :]
        hot = jnp.zeros((n_loc * cap, tok), F32)
        gate = jnp.zeros((n_loc * cap, tok), F32)
        for j in range(top_k):
            hit = keys[j:j + 1, :] == row_id
            hot = jnp.where(hit, 1.0, hot)
            gate = jnp.where(hit, gate_of[j:j + 1, :], gate)
        hot = hot.astype(BF)
        oh[q] = hot
        oht[q] = hot.T
        gr[q] = jnp.broadcast_to(jnp.sum(gate, axis=1, keepdims=True), gate.shape)

    def place_x(p, i):
        d, k = PASSES[p][i]
        q = FIRST[p] + i
        hot = oh[q]
        for n in range(d_model // COLS):
            cols = pl.ds(n * COLS, COLS)
            xv = dot(hot, xb[d, k, :, cols]).astype(BF)
            for e in range(n_loc):
                xr[e, pl.ds(q * cap, cap), cols] = xv[e * cap:(e + 1) * cap]

    def place_z(p, i):
        d, k = PASSES[p][i]
        q = FIRST[p] + i
        hot = oh[q]
        gate_row = jnp.concatenate([gr[q]] * (COLS // tok), axis=1)
        for n in range(d_model // COLS):
            cols = pl.ds(n * COLS, COLS)
            zv = (dot(hot, yb[d, k, :, cols]) * gate_row).astype(BF)
            for e in range(n_loc):
                zr[e, pl.ds(q * cap, cap), cols] = zv[e * cap:(e + 1) * cap]

    def place(p, i):
        place_x(p, i)
        place_z(p, i)

    def turn(src, dst):
        def one(e, carry):
            for n in range(src.shape[1] // COLS):
                cols = pl.ds(n * COLS, COLS)
                dst[e, :, cols] = src[e, cols, :].T
            return carry

        lax.fori_loop(0, n_loc, one, 0)

    def inner(p, e):
        at = pl.ds(FIRST[p] * cap, len(PASSES[p]) * cap)
        x_e = xr[e, at, :]
        z_e = zr[e, at, :]
        for n in range(d_ff // COLS):
            cols = pl.ds(n * COLS, COLS)
            a = dot(x_e, w1[e, :, cols]).astype(BF).astype(F32)
            b = dot(x_e, w3[e, :, cols]).astype(BF).astype(F32)
            dh = dot(z_e, w2t[e, :, cols])
            sg = jax.nn.sigmoid(a)
            act = a * sg
            hb[e, at, cols] = (act * b).astype(BF)
            dab[e, at, cols] = (dh * b * sg * (1.0 + a * (1.0 - sg))).astype(BF)
            dbb[e, at, cols] = (dh * act).astype(BF)

    def experts(p, lo, hi):
        lax.fori_loop(lo, hi, lambda e, c: (inner(p, e), c)[1], 0)

    def back(p, cols):
        rows = len(PASSES[p]) * cap
        at = pl.ds(FIRST[p] * cap, rows)

        def one(e, carry):
            dxb[e, pl.ds(0, rows), cols] = (
                dot(dab[e, at, :], w1t[e, :, cols]) + dot(dbb[e, at, :], w3t[e, :, cols])).astype(BF)
            return carry

        for e in range(n_loc):
            one(e, 0)

    sums = (own_out, part.at[0], osum, part.at[1], right_out, part.at[2], left_out, part.at[3])

    def combine(p, i, cols):
        q = FIRST[p] + i
        rows = jnp.concatenate([dxb[e, pl.ds(i * cap, cap), cols] for e in range(n_loc)], axis=0)
        sums[q][:, cols] = dot(oht[q], rows)

    def forward(i):
        x_r[i].wait_recv()
        x_f.append(send(xb.at[3, 0, halves[i]], xb.at[2, 0, halves[i]], right))
        y_l[i].wait_recv()
        y_f.append(send(yb.at[1, 0, halves[i]], yb.at[2, 0, halves[i]], left))

    n_cols = d_model // COLS
    chunks = [pl.ds(n * COLS, COLS) for n in range(n_cols)]
    x_f, y_f = [], []
    mask(0, 0)
    place(0, 0)
    loads[5].wait()
    turn(w2, w2t)
    m_m.wait_recv()
    mask(0, 1)
    x_m.wait_recv()
    y_m.wait_recv()
    place(0, 1)
    forward(0)
    loads[6].wait()
    turn(w1, w1t)
    loads[7].wait()
    turn(w3, w3t)
    forward(1)
    m_r.wait_recv()
    m_f = send(mb.at[3, 0], mb.at[2, 0], right)
    y_r = send(yb.at[0, 0], yb.at[3, 0], right)
    x_l = send(xb.at[0, 0], xb.at[1, 0], left)
    m_l.wait_recv()
    early = [
        send(mb.at[3, 0], mb.at[3, 1], mate),
        send(mb.at[1, 0], mb.at[1, 1], mate),
        send(xb.at[3, 0], xb.at[3, 1], mate),
        send(yb.at[1, 0], yb.at[1, 1], mate),
    ]
    experts(0, 0, n_loc)
    for cols in chunks:
        back(0, cols)
        combine(0, 1, cols)
    d_own = send(sums[1], ddr.at[0], mate)
    for cols in chunks:
        combine(0, 0, cols)
    for i in range(2):
        early[i].wait_recv()
    for i in range(4):
        mask(2, i)
    place_z(2, 0)
    place_x(2, 2)
    m_f.wait_recv()
    m_f2 = send(mb.at[2, 0], mb.at[2, 1], mate)
    mask(1, 0)

    opp = []
    for i, h in enumerate(halves):
        x_f[i].wait_recv()
        opp.append(send(xb.at[2, 0, h], xb.at[2, 1, h], mate))
        y_f[i].wait_recv()
        opp.append(send(yb.at[2, 0, h], yb.at[2, 1, h], mate))
    m_f2.wait_recv()
    mask(1, 1)
    place(1, 0)
    for c in opp:
        c.wait_recv()
    place(1, 1)
    experts(1, 0, n_loc)

    d_opp, hops = [], []

    def hop(n):
        cols = chunks[n]
        d_opp[n].wait_recv()
        osum[:, cols] += ddr[1, :, cols]
        hops.append((
            send(osum.at[pl.ds(0, half), cols], hopr.at[0, :, cols], right),
            send(osum.at[pl.ds(half, half), cols], hopr.at[1, :, cols], left)))

    for n, cols in enumerate(chunks):
        back(1, cols)
        combine(1, 1, cols)
        d_opp.append(send(sums[3].at[:, cols], ddr.at[1, :, cols], mate))
        combine(1, 0, cols)
        if n >= LAG:
            hop(n - LAG)
        if n == 1:
            y_r.wait_recv()
            y_r2 = send(yb.at[3, 0], yb.at[3, 1], mate)
            x_l.wait_recv()
            x_l2 = send(xb.at[1, 0], xb.at[1, 1], mate)
    for c in early[2:]:
        c.wait_recv()
    place_z(2, 1)
    hop(n_cols - 2)
    place_x(2, 3)
    place_x(2, 0)
    hop(n_cols - 1)
    place_z(2, 2)
    y_r2.wait_recv()
    x_l2.wait_recv()
    place_x(2, 1)
    place_z(2, 3)
    experts(2, 0, n_loc)

    d_side = []

    def side(n):
        cols = chunks[n]
        for c in d_side[n]:
            c.wait_recv()
        for c in hops[n]:
            c.wait_recv()
        near, far = pl.ds(0, half), pl.ds(half, half)
        right_out[near, cols] += ddr[2, near, cols] + hopr[0, :, cols]
        right_out[far, cols] += ddr[2, far, cols]
        left_out[near, cols] += ddr[3, near, cols]
        left_out[far, cols] += ddr[3, far, cols] + hopr[1, :, cols]

    for n, cols in enumerate(chunks):
        back(2, cols)
        combine(2, 1, cols)
        combine(2, 3, cols)
        d_side.append((
            send(sums[5].at[:, cols], ddr.at[2, :, cols], mate),
            send(sums[7].at[:, cols], ddr.at[3, :, cols], mate)))
        combine(2, 0, cols)
        combine(2, 2, cols)
        if n >= LAG:
            side(n - LAG)
    d_own.wait_recv()
    own_out[...] += ddr[0]
    for n in range(n_cols - LAG, n_cols):
        side(n)
    for c in made:
        c.wait_send()


def route(n_dev, cap, x, y, ids, slots, gates, w1, w2, w3):
    n_loc, d_model, d_ff = w1.shape
    top_k, tok = ids.shape
    n_rows = n_dev * cap
    hbm = pl.BlockSpec(memory_space=pltpu.HBM)
    vmem = pl.BlockSpec(memory_space=pltpu.VMEM)
    flops = 2 * n_loc * n_rows * d_model * d_ff * 5
    return pl.pallas_call(
        functools.partial(route_kernel, n_dev, cap),
        out_shape=(
            jax.ShapeDtypeStruct((n_loc, n_rows, d_model), BF),
            jax.ShapeDtypeStruct((n_loc, n_rows, d_model), BF),
            jax.ShapeDtypeStruct((n_loc, n_rows, d_ff), BF),
            jax.ShapeDtypeStruct((n_loc, n_rows, d_ff), BF),
            jax.ShapeDtypeStruct((n_loc, n_rows, d_ff), BF),
            jax.ShapeDtypeStruct((tok, d_model), F32),
            jax.ShapeDtypeStruct((tok, d_model), F32),
            jax.ShapeDtypeStruct((tok, d_model), F32),
        ),
        in_specs=[hbm] * 8,
        out_specs=[vmem] * 8,
        scratch_shapes=[
            pltpu.VMEM((4, 2, tok, d_model), BF),
            pltpu.VMEM((4, 2, tok, d_model), BF),
            pltpu.VMEM((4, 2, 2 * top_k, tok), F32),
            pltpu.VMEM(w1.shape, BF),
            pltpu.VMEM(w2.shape, BF),
            pltpu.VMEM(w3.shape, BF),
            pltpu.VMEM(w2.shape, BF),
            pltpu.VMEM(w1.shape, BF),
            pltpu.VMEM(w2.shape, BF),
            pltpu.VMEM((n_loc, 4 * cap, d_model), BF),
            pltpu.VMEM((8, n_loc * cap, tok), BF),
            pltpu.VMEM((8, tok, n_loc * cap), BF),
            pltpu.VMEM((8, n_loc * cap, tok), F32),
            pltpu.VMEM((4, tok, d_model), F32),
            pltpu.VMEM((4, tok, d_model), F32),
            pltpu.VMEM((2, tok // 2, d_model), F32),
            pltpu.VMEM((tok, d_model), F32),
            pltpu.VMEM((top_k, tok), jnp.int32),
            pltpu.VMEM((top_k, tok), jnp.int32),
            pltpu.VMEM((top_k, tok), F32),
            pltpu.SemaphoreType.DMA((56,)),
            pltpu.SemaphoreType.DMA((56,)),
            pltpu.SemaphoreType.DMA((8,)),
        ],
        compiler_params=pltpu.CompilerParams(
            collective_id=0, has_side_effects=True, vmem_limit_bytes=42000000),
        cost_estimate=pl.CostEstimate(flops=flops, bytes_accessed=14 * 1024 * 1024, transcendentals=0),
        name="route",
    )(*(pltpu.with_memory_space_constraint(v, pltpu.HBM) for v in (x, y, ids, slots, gates, w1, w2, w3)))


def grad_kernel(x_ref, z_ref, h_ref, da_ref, db_ref, g1_ref, g2_ref, g3_ref):
    x = x_ref[0]
    g1_ref[0] = dot(x, da_ref[0], 0, 0)
    g3_ref[0] = dot(x, db_ref[0], 0, 0)
    g2_ref[0] = dot(h_ref[0], z_ref[0], 0, 0)


def grads(xr, zr, h, da, db, parts=2):
    n_loc, n_rows, d_model = xr.shape
    d_ff = h.shape[2]
    bm, bf = d_model // parts, d_ff // parts
    full = lambda width: pl.BlockSpec((1, n_rows, width), lambda e, i: (e, 0, 0))
    part = lambda width: pl.BlockSpec((1, n_rows, width), lambda e, i: (e, 0, i))
    return pl.pallas_call(
        grad_kernel,
        grid=(n_loc, parts),
        in_specs=[part(bm), full(d_model), part(bf), full(d_ff), full(d_ff)],
        out_specs=[
            pl.BlockSpec((1, bm, d_ff), lambda e, i: (e, i, 0)),
            pl.BlockSpec((1, bf, d_model), lambda e, i: (e, i, 0)),
            pl.BlockSpec((1, bm, d_ff), lambda e, i: (e, i, 0)),
        ],
        out_shape=(
            jax.ShapeDtypeStruct((n_loc, d_model, d_ff), F32),
            jax.ShapeDtypeStruct((n_loc, d_ff, d_model), F32),
            jax.ShapeDtypeStruct((n_loc, d_model, d_ff), F32),
        ),
        compiler_params=pltpu.CompilerParams(
            dimension_semantics=("arbitrary", "arbitrary"), vmem_limit_bytes=20 * 1024 * 1024),
        cost_estimate=pl.CostEstimate(
            flops=6 * n_loc * n_rows * d_model * d_ff, bytes_accessed=26 * 1024 * 1024, transcendentals=0),
        name="grads",
    )(xr, zr, h, da, db)


def solution(mesh):
    n_dev = mesh.shape["ep"]
    n_chip = n_dev // 2
    to_right = [(i, ((i // 2 + 1) % n_chip) * 2 + i % 2) for i in range(n_dev)]
    to_left = [(j, i) for i, j in to_right]

    def local_step(x_loc, dy_loc, ids_loc, gate_loc, slot_loc, w_gate, w_down, w_up):
        tok_dev, top_k = ids_loc.shape
        n_exp = w_gate.shape[0] * n_dev
        cap = slot_capacity(tok_dev, top_k, n_exp)
        xr, zr, h, da, db, own, right, left = route(
            n_dev, cap, x_loc, dy_loc, ids_loc.T, slot_loc.T, gate_loc.T, w_gate, w_down, w_up)
        from_left = lax.ppermute(right, "ep", to_right)
        from_right = lax.ppermute(left, "ep", to_left)
        g_gate, g_down, g_up = grads(xr, zr, h, da, db)
        dx = (own + from_left + from_right).astype(BF)
        return dx, g_gate, g_down, g_up

    tok_spec = P(("dp", "ep"), None)
    w_spec = P("ep", None, None)
    grad_spec = P(("dp", "ep"), None, None)
    return jax.shard_map(
        local_step, mesh=mesh,
        in_specs=(tok_spec, tok_spec, tok_spec, tok_spec, tok_spec, w_spec, w_spec, w_spec),
        out_specs=(tok_spec, grad_spec, grad_spec, grad_spec), check_vma=False)
```

```python
import functools

import jax
import jax.numpy as jnp
from jax import lax
from jax.experimental import pallas as pl
from jax.experimental.pallas import tpu as pltpu
from jax.sharding import PartitionSpec as P

BF = jnp.bfloat16
F32 = jnp.float32
COLS = 256


def slot_capacity(tok_dev, top_k, n_exp):
    return ((3 * tok_dev * top_k) // (2 * n_exp) + 7) // 8 * 8


def dot(a, b, ca=1, cb=0):
    return lax.dot_general(a, b, (((ca,), (cb,)), ((), ())), preferred_element_type=F32)


PASSES = (((0, 0), (0, 1)), ((2, 0), (2, 1)), ((1, 0), (1, 1), (3, 0), (3, 1)))
FIRST = (0, 2, 4)
LAG = 2


def route_kernel(
    n_dev, cap, x_hbm, y_hbm, ids_hbm, slots_hbm, gates_hbm, w1_hbm, w2_hbm, w3_hbm,
    xr, zr, hb, dab, dbb, own_out, right_out, left_out,
    xb, yb, mb, w1, w2, w3, w1t, w2t, w3t, dxb, oh, oht, gr, part, ddr, hopr, osum, lead, landed, ids, slots, gates,
    send_sem, recv_sem, load_sem,
):
    n_chip = n_dev // 2
    me = lax.axis_index("ep")
    chip, core = me // 2, me % 2
    right = {"ep": ((chip + 1) % n_chip) * 2 + core}
    left = {"ep": ((chip + n_chip - 1) % n_chip) * 2 + core}
    mate = {"ep": chip * 2 + 1 - core}
    n_loc, d_model, d_ff = w1.shape
    top_k, tok = ids.shape
    half = tok // 2
    halves = (pl.ds(0, half), pl.ds(half, half))

    loads = [
        pltpu.make_async_copy(src, dst, load_sem.at[i])
        for i, (src, dst) in enumerate((
            (x_hbm, xb.at[0, 0]), (y_hbm, yb.at[0, 0]), (ids_hbm, ids), (slots_hbm, slots), (gates_hbm, gates),
            (w2_hbm, w2), (w1_hbm, w1), (w3_hbm, w3)))
    ]
    for c in loads[:5]:
        c.start()

    barrier = pltpu.get_barrier_semaphore()
    for peer in (right, left, mate):
        pl.semaphore_signal(barrier, inc=1, device_id=peer, device_id_type=pl.DeviceIdType.MESH)

    for c in loads[2:5]:
        c.wait()
    mb[0, 0, 0:top_k, :] = jnp.where(slots[...] >= 0, ids[...] * cap + slots[...], -1).astype(F32)
    mb[0, 0, top_k:2 * top_k, :] = gates[...]

    for c in loads[:2]:
        c.wait()
    for c in loads[5:]:
        c.start()
    pl.semaphore_wait(barrier, 3)

    made = []

    def send(src, dst, peer):
        n = len(made)
        c = pltpu.make_async_remote_copy(
            src_ref=src, dst_ref=dst, send_sem=send_sem.at[n], recv_sem=recv_sem.at[n],
            device_id=peer, device_id_type=pl.DeviceIdType.MESH)
        c.start()
        made.append(c)
        return c

    x_r, y_l = [], []
    for h in halves:
        x_r.append(send(xb.at[0, 0, h], xb.at[3, 0, h], right))
        y_l.append(send(yb.at[0, 0, h], yb.at[1, 0, h], left))
    x_m = send(xb.at[0, 0], xb.at[0, 1], mate)
    m_m = send(mb.at[0, 0], mb.at[0, 1], mate)
    y_m = send(yb.at[0, 0], yb.at[0, 1], mate)
    m_r = send(mb.at[0, 0], mb.at[3, 0], right)
    m_l = send(mb.at[0, 0], mb.at[1, 0], left)

    row_id = lax.broadcasted_iota(jnp.int32, (n_loc * cap, tok), 0) + me * (n_loc * cap)

    def mask(p, i):
        d, k = PASSES[p][i]
        q = FIRST[p] + i
        keys = mb[d, k, 0:top_k, :].astype(jnp.int32)
        gate_of = mb[d, k, top_k:2 * top_k, :]
        hot = jnp.zeros((n_loc * cap, tok), F32)
        gate = jnp.zeros((n_loc * cap, tok), F32)
        for j in range(top_k):
            hit = keys[j:j + 1, :] == row_id
            hot = jnp.where(hit, 1.0, hot)
            gate = jnp.where(hit, gate_of[j:j + 1, :], gate)
        hot = hot.astype(BF)
        oh[q] = hot
        oht[q] = hot.T
        gr[q] = jnp.broadcast_to(jnp.sum(gate, axis=1, keepdims=True), gate.shape)

    def place_x(p, i):
        d, k = PASSES[p][i]
        q = FIRST[p] + i
        hot = oh[q]
        for n in range(d_model // COLS):
            cols = pl.ds(n * COLS, COLS)
            xv = dot(hot, xb[d, k, :, cols]).astype(BF)
            for e in range(n_loc):
                xr[e, pl.ds(q * cap, cap), cols] = xv[e * cap:(e + 1) * cap]

    def place_z(p, i):
        d, k = PASSES[p][i]
        q = FIRST[p] + i
        hot = oh[q]
        gate_row = jnp.concatenate([gr[q]] * (COLS // tok), axis=1)
        for n in range(d_model // COLS):
            cols = pl.ds(n * COLS, COLS)
            zv = (dot(hot, yb[d, k, :, cols]) * gate_row).astype(BF)
            for e in range(n_loc):
                zr[e, pl.ds(q * cap, cap), cols] = zv[e * cap:(e + 1) * cap]

    def place(p, i):
        place_x(p, i)
        place_z(p, i)

    def turn(src, dst):
        def one(e, carry):
            for n in range(src.shape[1] // COLS):
                cols = pl.ds(n * COLS, COLS)
                dst[e, :, cols] = src[e, cols, :].T
            return carry

        lax.fori_loop(0, n_loc, one, 0)

    def inner(p, e):
        at = pl.ds(FIRST[p] * cap, len(PASSES[p]) * cap)
        x_e = xr[e, at, :]
        z_e = zr[e, at, :]
        for n in range(d_ff // COLS):
            cols = pl.ds(n * COLS, COLS)
            a = dot(x_e, w1[e, :, cols]).astype(BF).astype(F32)
            b = dot(x_e, w3[e, :, cols]).astype(BF).astype(F32)
            dh = dot(z_e, w2t[e, :, cols])
            sg = jax.nn.sigmoid(a)
            act = a * sg
            hb[e, at, cols] = (act * b).astype(BF)
            dab[e, at, cols] = (dh * b * sg * (1.0 + a * (1.0 - sg))).astype(BF)
            dbb[e, at, cols] = (dh * act).astype(BF)

    def experts(p, lo, hi):
        lax.fori_loop(lo, hi, lambda e, c: (inner(p, e), c)[1], 0)

    def back(p, cols):
        rows = len(PASSES[p]) * cap
        at = pl.ds(FIRST[p] * cap, rows)

        def one(e, carry):
            dxb[e, pl.ds(0, rows), cols] = (
                dot(dab[e, at, :], w1t[e, :, cols]) + dot(dbb[e, at, :], w3t[e, :, cols])).astype(BF)
            return carry

        for e in range(n_loc):
            one(e, 0)

    sums = (own_out, part.at[0], osum, part.at[1], None, part.at[2], None, part.at[3])

    def outward(side, n):
        if n == 0:
            return lead.at[side]
        return (right_out, left_out)[side].at[:, pl.ds((n - 1) * COLS, COLS)]

    def combine(p, i, cols, n=None):
        q = FIRST[p] + i
        rows = jnp.concatenate([dxb[e, pl.ds(i * cap, cap), cols] for e in range(n_loc)], axis=0)
        if n is None:
            sums[q][:, cols] = dot(oht[q], rows)
        else:
            outward(i // 2, n)[...] = dot(oht[q], rows)

    def forward(i):
        x_r[i].wait_recv()
        x_f.append(send(xb.at[3, 0, halves[i]], xb.at[2, 0, halves[i]], right))
        y_l[i].wait_recv()
        y_f.append(send(yb.at[1, 0, halves[i]], yb.at[2, 0, halves[i]], left))

    n_cols = d_model // COLS
    chunks = [pl.ds(n * COLS, COLS) for n in range(n_cols)]
    x_f, y_f = [], []
    mask(0, 0)
    place(0, 0)
    loads[5].wait()
    turn(w2, w2t)
    m_m.wait_recv()
    mask(0, 1)
    x_m.wait_recv()
    y_m.wait_recv()
    place(0, 1)
    forward(0)
    loads[6].wait()
    turn(w1, w1t)
    loads[7].wait()
    turn(w3, w3t)
    forward(1)
    m_r.wait_recv()
    m_f = send(mb.at[3, 0], mb.at[2, 0], right)
    y_r = send(yb.at[0, 0], yb.at[3, 0], right)
    x_l = send(xb.at[0, 0], xb.at[1, 0], left)
    m_l.wait_recv()
    early = [
        send(mb.at[3, 0], mb.at[3, 1], mate),
        send(mb.at[1, 0], mb.at[1, 1], mate),
        send(xb.at[3, 0], xb.at[3, 1], mate),
        send(yb.at[1, 0], yb.at[1, 1], mate),
    ]
    experts(0, 0, n_loc)
    for cols in chunks:
        back(0, cols)
        combine(0, 1, cols)
    d_own = send(sums[1], ddr.at[0], mate)
    for cols in chunks:
        combine(0, 0, cols)
    for i in range(2):
        early[i].wait_recv()
    for i in range(4):
        mask(2, i)
    place_z(2, 0)
    place_x(2, 2)
    m_f.wait_recv()
    m_f2 = send(mb.at[2, 0], mb.at[2, 1], mate)
    mask(1, 0)

    opp = []
    for i, h in enumerate(halves):
        x_f[i].wait_recv()
        opp.append(send(xb.at[2, 0, h], xb.at[2, 1, h], mate))
        y_f[i].wait_recv()
        opp.append(send(yb.at[2, 0, h], yb.at[2, 1, h], mate))
    m_f2.wait_recv()
    mask(1, 1)
    place(1, 0)
    for c in opp:
        c.wait_recv()
    place(1, 1)
    experts(1, 0, n_loc)

    d_opp, hops = [], []

    def hop(n):
        cols = chunks[n]
        d_opp[n].wait_recv()
        osum[:, cols] += ddr[1, :, cols]
        hops.append((
            send(osum.at[pl.ds(0, half), cols], hopr.at[0, :, cols], right),
            send(osum.at[pl.ds(half, half), cols], hopr.at[1, :, cols], left)))

    for n, cols in enumerate(chunks):
        back(1, cols)
        combine(1, 1, cols)
        d_opp.append(send(sums[3].at[:, cols], ddr.at[1, :, cols], mate))
        combine(1, 0, cols)
        if n >= LAG:
            hop(n - LAG)
        if n == 1:
            y_r.wait_recv()
            y_r2 = send(yb.at[3, 0], yb.at[3, 1], mate)
            x_l.wait_recv()
            x_l2 = send(xb.at[1, 0], xb.at[1, 1], mate)
    for c in early[2:]:
        c.wait_recv()
    place_z(2, 1)
    hop(n_cols - 2)
    place_x(2, 3)
    place_x(2, 0)
    hop(n_cols - 1)
    place_z(2, 2)
    y_r2.wait_recv()
    x_l2.wait_recv()
    place_x(2, 1)
    place_z(2, 3)
    experts(2, 0, n_loc)

    d_side = []

    def side(n):
        cols = chunks[n]
        for c in d_side[n]:
            c.wait_recv()
        for c in hops[n]:
            c.wait_recv()
        near, far = pl.ds(0, half), pl.ds(half, half)
        to_r, to_l = outward(0, n), outward(1, n)
        to_r[near, :] += ddr[2, near, cols] + hopr[0, :, cols]
        to_r[far, :] += ddr[2, far, cols]
        to_l[near, :] += ddr[3, near, cols]
        to_l[far, :] += ddr[3, far, cols] + hopr[1, :, cols]

    for n, cols in enumerate(chunks):
        back(2, cols)
        combine(2, 1, cols)
        combine(2, 3, cols)
        d_side.append((
            send(sums[5].at[:, cols], ddr.at[2, :, cols], mate),
            send(sums[7].at[:, cols], ddr.at[3, :, cols], mate)))
        combine(2, 0, cols, n)
        combine(2, 2, cols, n)
        if n == 1:
            side(0)
            last = [send(lead.at[0], landed.at[0], right), send(lead.at[1], landed.at[1], left)]
    d_own.wait_recv()
    own_out[...] += ddr[0]
    for n in range(1, n_cols):
        side(n)
    for c in last:
        c.wait_recv()
    own_out[:, chunks[0]] += landed[0] + landed[1]
    for c in made:
        c.wait_send()


def route(n_dev, cap, x, y, ids, slots, gates, w1, w2, w3):
    n_loc, d_model, d_ff = w1.shape
    top_k, tok = ids.shape
    n_rows = n_dev * cap
    hbm = pl.BlockSpec(memory_space=pltpu.HBM)
    vmem = pl.BlockSpec(memory_space=pltpu.VMEM)
    flops = 2 * n_loc * n_rows * d_model * d_ff * 5
    return pl.pallas_call(
        functools.partial(route_kernel, n_dev, cap),
        out_shape=(
            jax.ShapeDtypeStruct((n_loc, n_rows, d_model), BF),
            jax.ShapeDtypeStruct((n_loc, n_rows, d_model), BF),
            jax.ShapeDtypeStruct((n_loc, n_rows, d_ff), BF),
            jax.ShapeDtypeStruct((n_loc, n_rows, d_ff), BF),
            jax.ShapeDtypeStruct((n_loc, n_rows, d_ff), BF),
            jax.ShapeDtypeStruct((tok, d_model), F32),
            jax.ShapeDtypeStruct((tok, d_model - COLS), F32),
            jax.ShapeDtypeStruct((tok, d_model - COLS), F32),
        ),
        in_specs=[hbm] * 8,
        out_specs=[vmem] * 8,
        scratch_shapes=[
            pltpu.VMEM((4, 2, tok, d_model), BF),
            pltpu.VMEM((4, 2, tok, d_model), BF),
            pltpu.VMEM((4, 2, 2 * top_k, tok), F32),
            pltpu.VMEM(w1.shape, BF),
            pltpu.VMEM(w2.shape, BF),
            pltpu.VMEM(w3.shape, BF),
            pltpu.VMEM(w2.shape, BF),
            pltpu.VMEM(w1.shape, BF),
            pltpu.VMEM(w2.shape, BF),
            pltpu.VMEM((n_loc, 4 * cap, d_model), BF),
            pltpu.VMEM((8, n_loc * cap, tok), BF),
            pltpu.VMEM((8, tok, n_loc * cap), BF),
            pltpu.VMEM((8, n_loc * cap, tok), F32),
            pltpu.VMEM((4, tok, d_model), F32),
            pltpu.VMEM((4, tok, d_model), F32),
            pltpu.VMEM((2, tok // 2, d_model), F32),
            pltpu.VMEM((tok, d_model), F32),
            pltpu.VMEM((2, tok, COLS), F32),
            pltpu.VMEM((2, tok, COLS), F32),
            pltpu.VMEM((top_k, tok), jnp.int32),
            pltpu.VMEM((top_k, tok), jnp.int32),
            pltpu.VMEM((top_k, tok), F32),
            pltpu.SemaphoreType.DMA((56,)),
            pltpu.SemaphoreType.DMA((56,)),
            pltpu.SemaphoreType.DMA((8,)),
        ],
        compiler_params=pltpu.CompilerParams(
            collective_id=0, has_side_effects=True, vmem_limit_bytes=42400000),
        cost_estimate=pl.CostEstimate(flops=flops, bytes_accessed=14 * 1024 * 1024, transcendentals=0),
        name="route",
    )(*(pltpu.with_memory_space_constraint(v, pltpu.HBM) for v in (x, y, ids, slots, gates, w1, w2, w3)))


def grad_kernel(x_ref, z_ref, h_ref, da_ref, db_ref, g1_ref, g2_ref, g3_ref):
    x = x_ref[0]
    g1_ref[0] = dot(x, da_ref[0], 0, 0)
    g3_ref[0] = dot(x, db_ref[0], 0, 0)
    g2_ref[0] = dot(h_ref[0], z_ref[0], 0, 0)


def grads(xr, zr, h, da, db, parts=2):
    n_loc, n_rows, d_model = xr.shape
    d_ff = h.shape[2]
    bm, bf = d_model // parts, d_ff // parts
    full = lambda width: pl.BlockSpec((1, n_rows, width), lambda e, i: (e, 0, 0))
    part = lambda width: pl.BlockSpec((1, n_rows, width), lambda e, i: (e, 0, i))
    return pl.pallas_call(
        grad_kernel,
        grid=(n_loc, parts),
        in_specs=[part(bm), full(d_model), part(bf), full(d_ff), full(d_ff)],
        out_specs=[
            pl.BlockSpec((1, bm, d_ff), lambda e, i: (e, i, 0)),
            pl.BlockSpec((1, bf, d_model), lambda e, i: (e, i, 0)),
            pl.BlockSpec((1, bm, d_ff), lambda e, i: (e, i, 0)),
        ],
        out_shape=(
            jax.ShapeDtypeStruct((n_loc, d_model, d_ff), F32),
            jax.ShapeDtypeStruct((n_loc, d_ff, d_model), F32),
            jax.ShapeDtypeStruct((n_loc, d_model, d_ff), F32),
        ),
        compiler_params=pltpu.CompilerParams(
            dimension_semantics=("arbitrary", "arbitrary"), vmem_limit_bytes=20 * 1024 * 1024),
        cost_estimate=pl.CostEstimate(
            flops=6 * n_loc * n_rows * d_model * d_ff, bytes_accessed=26 * 1024 * 1024, transcendentals=0),
        name="grads",
    )(xr, zr, h, da, db)


def solution(mesh):
    n_dev = mesh.shape["ep"]
    n_chip = n_dev // 2
    to_right = [(i, ((i // 2 + 1) % n_chip) * 2 + i % 2) for i in range(n_dev)]
    to_left = [(j, i) for i, j in to_right]

    def local_step(x_loc, dy_loc, ids_loc, gate_loc, slot_loc, w_gate, w_down, w_up):
        tok_dev, top_k = ids_loc.shape
        n_exp = w_gate.shape[0] * n_dev
        cap = slot_capacity(tok_dev, top_k, n_exp)
        xr, zr, h, da, db, own, right, left = route(
            n_dev, cap, x_loc, dy_loc, ids_loc.T, slot_loc.T, gate_loc.T, w_gate, w_down, w_up)
        from_left = lax.ppermute(right, "ep", to_right)
        from_right = lax.ppermute(left, "ep", to_left)
        g_gate, g_down, g_up = grads(xr, zr, h, da, db)
        dx = (own + jnp.pad(from_left + from_right, ((0, 0), (COLS, 0)))).astype(BF)
        return dx, g_gate, g_down, g_up

    tok_spec = P(("dp", "ep"), None)
    w_spec = P("ep", None, None)
    grad_spec = P(("dp", "ep"), None, None)
    return jax.shard_map(
        local_step, mesh=mesh,
        in_specs=(tok_spec, tok_spec, tok_spec, tok_spec, tok_spec, w_spec, w_spec, w_spec),
        out_specs=(tok_spec, grad_spec, grad_spec, grad_spec), check_vma=False)
```
